32 devices in a mesh: dp: 8 (over z, y), expert: 4 (over x, core).
Axes of the slice: x: 2, y: 2, z: 4, core: 2. Of those that a mesh axis runs over, the one named last changes fastest.
Arguments:
- expert_grads: bfloat16 [8, 4, 1024, 896], P('dp', 'expert'), may hold values from -768 to 768
- round_offsets: int32 [8, 4, 1024], P('dp', 'expert'), may hold values from 0 to 1073741823
- slot_expert: int32 [4], replicated, may hold values from 0 to 3, each once
- master_weight: float32 [4, 1024, 896], P('expert', 'dp'), may hold values from -0.1875 to 0.1875
Outputs:
- mean_grad: float32 [4, 1024, 896], P('expert', 'dp')
- new_weight: float32 [4, 1024, 896], P('expert', 'dp')
- block_step: float32 [4, 8], P('expert', 'dp')
The draws below stay inside these ranges and needn't reach their ends.
Inputs may be any that keep to these rules, and one draw needn't show every extreme that they name: `slot_expert`: each of 0 to 3 appears once.
All inputs are finite; a program needn't handle non-finite values.
Results may differ from the reference program's by a relative error of at most 0.0003.
Values may be sent and summed in bfloat16 or wider, within the bound.
No kernel may reach another device: no remote copies, remote signals or barrier semaphores. Data moves between devices by JAX's collectives and lax.ppermute only.
A program may use at most 64 MiB of HBM per device.

```python
import jax
import jax.numpy as jnp
from jax import lax

D = 1024
FF = 896
EXPERTS = 4
REPLICAS = 8
N_DP = 8


def draw_expert_grads(key, part):
    base_key = jax.random.fold_in(key, 11)
    scale_key = jax.random.fold_in(key, 12)
    pair_key = jax.random.fold_in(key, 13)
    block_count = REPLICAS
    block_rows = D // REPLICAS
    base = jnp.clip(jax.random.normal(base_key, (REPLICAS, EXPERTS, D, FF), jnp.float32), -4.0, 4.0)
    block_scale = jnp.exp(jax.random.uniform(scale_key, (EXPERTS, block_count), jnp.float32, jnp.log(0.5), jnp.log(32.0)))
    row_scale = jnp.repeat(block_scale, block_rows, axis=1)
    paired = jax.random.permutation(pair_key, block_count)
    blocks_iota = jnp.arange(block_count)
    spike = jnp.where(blocks_iota[None, :] == paired[:, None], jnp.float32(6.0), jnp.float32(1.0))
    row_spike = jnp.repeat(spike, block_rows, axis=1)
    values = base * row_scale[None, :, :, None] * row_spike[:, None, :, None]
    return values.astype(jnp.bfloat16)


def with_ends(drawn, own_key, smallest, high):
    longest = drawn.shape.index(max(drawn.shape))
    spots = []
    for shift in (0, 1):
        where = [jax.random.randint(jax.random.fold_in(own_key, axis), (), 0, length) for axis, length in enumerate(drawn.shape)]
        where[longest] = (where[longest] + shift) % drawn.shape[longest]
        spots.append(tuple(where))
    return drawn.at[spots[0]].set(smallest).at[spots[1]].set(high)


def steps_of(own_key, extent, pieces, smallest, top_value):
    gain = 1.0
    for dim, blocks in pieces:
        draws = jax.random.uniform(jax.random.fold_in(jax.random.fold_in(own_key, 6), dim), (blocks,), jnp.float32, smallest / len(pieces), top_value / len(pieces))
        gain = gain * jnp.repeat(jnp.exp(draws), extent[dim] // blocks).reshape((-1,) + (1,) * (len(extent) - 1 - dim))
    return gain


def gaussian(key, shape, deviation, limit, pieces=(), held_as=jnp.bfloat16):
    level = steps_of(key, shape, pieces, -0.22, 0.18) if pieces else 1.0
    values = jax.random.normal(key, shape, jnp.float32) * deviation * level
    return jnp.minimum(jnp.maximum(values, -limit), limit).astype(held_as)


def setup_inputs(seed: int = 0) -> dict:
    key_of = jax.random.split(jax.random.key(seed), 5)
    return {
        "expert_grads": draw_expert_grads(jax.random.fold_in(key_of[4], 71), 0),
        "round_offsets": with_ends(jax.random.randint(key_of[1], (REPLICAS, EXPERTS, D), 0, 2 ** 30), jax.random.fold_in(key_of[1], 1), 0, (2 ** 30) - 1).astype(jnp.int32),
        "slot_expert": jax.random.permutation(key_of[2], EXPERTS).astype(jnp.int32),
        "master_weight": gaussian(key_of[3], (EXPERTS, D, FF), D ** -0.5, 0.1875, ((0, 4), (1, 8)), jnp.float32),
    }


level_bits = 6
low_power = -30
high_power = 30
learn_rate = 0.05


def power_steps(maxima):
    powers = jnp.array([2.0 ** exponent for exponent in range(low_power, high_power)], jnp.float32)
    reached = maxima[..., None] >= powers
    doubled = jnp.prod(jnp.where(reached, jnp.float32(2.0), jnp.float32(1.0)), axis=-1)
    return (2.0 ** (low_power - level_bits)) * doubled


def dither(element_code):
    mixed = element_code * 747796405 + 1013904223
    mixed = jnp.bitwise_xor(mixed, jnp.right_shift(mixed, 13))
    mixed = mixed * 1103515245
    mixed = jnp.bitwise_xor(mixed, jnp.right_shift(mixed, 16))
    return jnp.bitwise_and(jnp.right_shift(mixed, 12), 255).astype(jnp.float32) / 256.0


def quantize(values, inverse_step, offsets):
    columns = lax.broadcasted_iota(jnp.int32, (1, values.shape[-1]), 1)
    element_code = offsets.astype(jnp.int32)[..., None] + columns
    scaled = values * inverse_step
    floor_part = jnp.floor(scaled)
    return (floor_part + jnp.floor((scaled - floor_part) + dither(element_code))).astype(jnp.int32)


def reference(expert_grads, round_offsets, slot_expert, master_weight):
    slot_count = expert_grads.shape[1]
    row_count = expert_grads.shape[2]
    hidden = expert_grads.shape[3]
    blocks = N_DP
    block_rows = row_count // blocks

    def max_step(running, grads_one):
        shaped = jnp.abs(grads_one).reshape(slot_count, blocks, block_rows, hidden)
        return jnp.maximum(running, jnp.max(shaped, axis=(2, 3)).astype(jnp.float32)), None

    maxima, ignored = lax.scan(max_step, jnp.zeros((slot_count, blocks), jnp.float32), expert_grads)
    step_sizes = power_steps(maxima)
    inverse_step = (1.0 / step_sizes)[:, :, None, None]

    def sum_step(running, grads_pair):
        grads_one, offsets_one = grads_pair
        shaped = grads_one.astype(jnp.float32).reshape(slot_count, blocks, block_rows, hidden)
        offsets_shaped = offsets_one.reshape(slot_count, blocks, block_rows)
        counts = quantize(shaped, inverse_step, offsets_shaped).reshape(slot_count, row_count, hidden)
        return running + counts, None

    totals, ignored = lax.scan(sum_step, jnp.zeros((slot_count, row_count, hidden), jnp.int32), (expert_grads, round_offsets))
    shaped_totals = totals.astype(jnp.float32).reshape(slot_count, blocks, block_rows, hidden)
    mean_slot = (shaped_totals * (step_sizes / N_DP)[:, :, None, None]).reshape(slot_count, row_count, hidden)
    inverse_order = jnp.argsort(slot_expert).astype(jnp.int32)
    mean_grad = mean_slot[inverse_order]
    block_step = step_sizes[inverse_order]
    new_weight = master_weight - learn_rate * mean_grad
    return mean_grad, new_weight, block_step
```

```python
import itertools

import jax
import jax.numpy as jnp
from jax import lax
from jax.sharding import PartitionSpec as P

level_bits = 6
low_power = -30
high_power = 30
learn_rate = 0.05
field_base = 32768
count_shift = 64
square = 4


def power_steps(maxima):
    powers = jnp.array([2.0**exponent for exponent in range(low_power, high_power)], jnp.float32)
    reached = maxima[..., None] >= powers
    doubled = jnp.prod(jnp.where(reached, jnp.float32(2.0), jnp.float32(1.0)), axis=-1)
    return 2.0 ** (low_power - level_bits) * doubled


def dither(element_code):
    mixed = element_code * 747796405 + 1013904223
    mixed = jnp.bitwise_xor(mixed, jnp.right_shift(mixed, 13))
    mixed = mixed * 1103515245
    mixed = jnp.bitwise_xor(mixed, jnp.right_shift(mixed, 16))
    return jnp.bitwise_and(jnp.right_shift(mixed, 12), 255).astype(jnp.float32) / 256.0


def quantize(values, inverse_step, offsets):
    columns = lax.broadcasted_iota(jnp.int32, (1, values.shape[-1]), 1)
    element_code = offsets[..., None] + columns
    scaled = values.astype(jnp.float32) * inverse_step
    floor_part = jnp.floor(scaled)
    return floor_part + jnp.floor(scaled - floor_part + dither(element_code))


def apply_update(mean_grad, master_weight):
    return mean_grad, master_weight - learn_rate * mean_grad


def general_body(expert_grads, round_offsets, slot_expert, master_weight):
    dp_count = lax.axis_size("dp")
    local_grads = expert_grads[0]
    slot_count, row_count, hidden = local_grads.shape
    block_rows = row_count // dp_count
    shaped = local_grads.reshape(slot_count, dp_count, block_rows, hidden)
    maxima = lax.pmax(jnp.max(jnp.abs(shaped), axis=(2, 3)).astype(jnp.float32), "dp")
    all_steps = power_steps(maxima)
    counts = quantize(
        shaped,
        (1.0 / all_steps)[:, :, None, None],
        round_offsets[0].reshape(slot_count, dp_count, block_rows),
    ).astype(jnp.int32).reshape(slot_count, row_count, hidden)
    half = hidden // 2
    words = (counts[:, :, :half] + count_shift) * field_base + (counts[:, :, half:] + count_shift)
    summed = lax.psum_scatter(words, "dp", scatter_dimension=1, tiled=True)
    upper = jnp.right_shift(summed, 15) - count_shift * dp_count
    lower = jnp.bitwise_and(summed, field_base - 1) - count_shift * dp_count
    totals = jnp.concatenate([upper, lower], axis=2)
    step_sizes = lax.dynamic_slice_in_dim(all_steps, lax.axis_index("dp"), 1, 1)
    mean_slot = totals.astype(jnp.float32) * (step_sizes / dp_count)[..., None]
    gathered = lax.all_gather(mean_slot, "expert", axis=0, tiled=True)
    gathered_steps = lax.all_gather(step_sizes, "expert", axis=0, tiled=True)
    wanted = lax.axis_index("expert") * slot_count + lax.broadcasted_iota(
        jnp.int32, (slot_count, 1), 0
    )
    positions = lax.broadcasted_iota(jnp.int32, (1, slot_expert.shape[0]), 1)
    holder = jnp.sum(jnp.where(slot_expert[None, :] == wanted, positions, 0), axis=1)
    mean_grad, new_weight = apply_update(gathered[holder], master_weight)
    return mean_grad, new_weight, gathered_steps[holder]


def flips(count, mask):
    return [(index, index ^ mask) for index in range(count)]


def staged_body(expert_grads, round_offsets, slot_expert, master_weight):
    dp_count = lax.axis_size("dp")
    expert_count = lax.axis_size("expert")
    row_count, hidden = expert_grads.shape[2:]
    block_rows = row_count // dp_count
    groups = dp_count // square
    me = lax.axis_index("dp")
    blocks = expert_grads[0, 0].reshape(dp_count, block_rows, hidden)
    offsets = round_offsets[0, 0].reshape(dp_count, block_rows)

    def pick(array, index):
        return lax.dynamic_index_in_dim(array, index, 0, keepdims=False)

    raw = [[None] * square for _ in range(groups)]
    codes = [[None] * square for _ in range(groups)]
    for near in range(square):
        for far in reversed(range(groups)):
            target = (me ^ near) ^ (far * square)
            rows, seeds = pick(blocks, target), pick(offsets, target)
            if near:
                rows = lax.ppermute(rows, "dp", flips(dp_count, near))
                seeds = lax.ppermute(seeds, "dp", flips(dp_count, near))
            raw[far][near], codes[far][near] = rows, seeds

    peaks = jnp.stack(
        [
            jnp.max(jnp.stack([jnp.max(jnp.abs(rows)) for rows in raw[far]])).astype(jnp.float32)
            for far in range(groups)
        ]
    )
    shared = peaks
    for far in range(1, groups):
        order = jnp.array([block ^ far for block in range(groups)])
        shared = jnp.maximum(shared, lax.ppermute(peaks, "dp", flips(dp_count, far * square))[order])
    steps = power_steps(shared)

    partial = []
    for far in range(groups):
        total = sum(
            quantize(raw[far][near], 1.0 / steps[far], codes[far][near]) for near in range(square)
        )
        partial.append(total.astype(jnp.bfloat16))
    step_rows = jnp.full((1, 128), steps[0], jnp.float32)

    orders = list(itertools.permutations(range(expert_count)))
    match = [
        jnp.all(slot_expert == jnp.array(order, jnp.int32)).astype(jnp.int32) * number
        for number, order in enumerate(orders)
    ]

    def route(order):
        def send(operands):
            parts, step_part = operands
            out = []
            for far in reversed(range(groups)):
                pairs = [
                    (block * expert_count + slot, (block ^ (far * square)) * expert_count + order[slot])
                    for block in range(dp_count)
                    for slot in range(expert_count)
                ]
                out.append(lax.ppermute(parts[far], ("dp", "expert"), pairs))
                if far == 0:
                    step_part = lax.ppermute(step_part, ("dp", "expert"), pairs)
            return tuple(out), step_part

        return send

    received, step_row = lax.switch(sum(match), [route(order) for order in orders], (partial, step_rows))
    totals = sum(part.astype(jnp.float32) for part in received)
    step = step_row[0, 0]
    mean_grad, new_weight = apply_update((totals * (step / dp_count))[None], master_weight)
    return mean_grad, new_weight, step.reshape(1, 1)


def solution(mesh):
    dp_count, expert_count = mesh.shape["dp"], mesh.shape["expert"]

    def body(expert_grads, round_offsets, slot_expert, master_weight):
        staged = (
            dp_count in (4, 8, 16)
            and expert_count <= 4
            and expert_grads.shape[1] == 1
            and expert_grads.shape[2] % (8 * dp_count) == 0
        )
        chosen = staged_body if staged else general_body
        return chosen(expert_grads, round_offsets, slot_expert, master_weight)

    return jax.shard_map(
        body,
        mesh=mesh,
        in_specs=(
            P("dp", "expert", None, None),
            P("dp", "expert", None),
            P(),
            P("expert", "dp", None),
        ),
        out_specs=(P("expert", "dp", None), P("expert", "dp", None), P("expert", "dp")),
        check_vma=False,
    )
```

```python
import itertools

import jax
import jax.numpy as jnp
from jax import lax
from jax.sharding import PartitionSpec as P

level_bits = 6
low_power = -30
high_power = 30
learn_rate = 0.05
field_base = 32768
count_shift = 64
square = 4


def power_steps(maxima):
    powers = jnp.array([2.0**exponent for exponent in range(low_power, high_power)], jnp.float32)
    reached = maxima[..., None] >= powers
    doubled = jnp.prod(jnp.where(reached, jnp.float32(2.0), jnp.float32(1.0)), axis=-1)
    return 2.0 ** (low_power - level_bits) * doubled


def dither(element_code):
    mixed = element_code * 747796405 + 1013904223
    mixed = jnp.bitwise_xor(mixed, jnp.right_shift(mixed, 13))
    mixed = mixed * 1103515245
    mixed = jnp.bitwise_xor(mixed, jnp.right_shift(mixed, 16))
    return jnp.bitwise_and(jnp.right_shift(mixed, 12), 255).astype(jnp.float32) / 256.0


def quantize(values, inverse_step, offsets):
    columns = lax.broadcasted_iota(jnp.int32, (1, values.shape[-1]), 1)
    element_code = offsets[..., None] + columns
    scaled = values.astype(jnp.float32) * inverse_step
    floor_part = jnp.floor(scaled)
    return floor_part + jnp.floor(scaled - floor_part + dither(element_code))


def apply_update(mean_grad, master_weight):
    return mean_grad, master_weight - learn_rate * mean_grad


def general_body(expert_grads, round_offsets, slot_expert, master_weight):
    dp_count = lax.axis_size("dp")
    local_grads = expert_grads[0]
    slot_count, row_count, hidden = local_grads.shape
    block_rows = row_count // dp_count
    shaped = local_grads.reshape(slot_count, dp_count, block_rows, hidden)
    maxima = lax.pmax(jnp.max(jnp.abs(shaped), axis=(2, 3)).astype(jnp.float32), "dp")
    all_steps = power_steps(maxima)
    counts = quantize(
        shaped,
        (1.0 / all_steps)[:, :, None, None],
        round_offsets[0].reshape(slot_count, dp_count, block_rows),
    ).astype(jnp.int32).reshape(slot_count, row_count, hidden)
    half = hidden // 2
    words = (counts[:, :, :half] + count_shift) * field_base + (counts[:, :, half:] + count_shift)
    summed = lax.psum_scatter(words, "dp", scatter_dimension=1, tiled=True)
    upper = jnp.right_shift(summed, 15) - count_shift * dp_count
    lower = jnp.bitwise_and(summed, field_base - 1) - count_shift * dp_count
    totals = jnp.concatenate([upper, lower], axis=2)
    step_sizes = lax.dynamic_slice_in_dim(all_steps, lax.axis_index("dp"), 1, 1)
    mean_slot = totals.astype(jnp.float32) * (step_sizes / dp_count)[..., None]
    gathered = lax.all_gather(mean_slot, "expert", axis=0, tiled=True)
    gathered_steps = lax.all_gather(step_sizes, "expert", axis=0, tiled=True)
    wanted = lax.axis_index("expert") * slot_count + lax.broadcasted_iota(
        jnp.int32, (slot_count, 1), 0
    )
    positions = lax.broadcasted_iota(jnp.int32, (1, slot_expert.shape[0]), 1)
    holder = jnp.sum(jnp.where(slot_expert[None, :] == wanted, positions, 0), axis=1)
    mean_grad, new_weight = apply_update(gathered[holder], master_weight)
    return mean_grad, new_weight, gathered_steps[holder]


def flips(count, mask):
    return [(index, index ^ mask) for index in range(count)]


def staged_body(expert_grads, round_offsets, slot_expert, master_weight):
    dp_count = lax.axis_size("dp")
    expert_count = lax.axis_size("expert")
    row_count, hidden = expert_grads.shape[2:]
    block_rows = row_count // dp_count
    groups = dp_count // square
    me = lax.axis_index("dp")
    blocks = expert_grads[0, 0].reshape(dp_count, block_rows, hidden)
    offsets = round_offsets[0, 0].reshape(dp_count, block_rows)

    def pick(array, index):
        return lax.dynamic_index_in_dim(array, index, 0, keepdims=False)

    raw, codes = [], []
    for near in range(square):
        picked = [(me ^ near) ^ (far * square) for far in range(groups)]
        rows = jnp.stack([pick(blocks, target) for target in picked])
        seeds = jnp.stack([pick(offsets, target) for target in picked])
        if near:
            rows = lax.ppermute(rows, "dp", flips(dp_count, near))
            seeds = lax.ppermute(seeds, "dp", flips(dp_count, near))
        raw.append(rows)
        codes.append(seeds)

    peaks = raw[0]
    for rows in raw[1:]:
        peaks = jnp.maximum(jnp.abs(peaks), jnp.abs(rows))
    peaks = jnp.max(peaks, axis=(1, 2)).astype(jnp.float32)
    shared = peaks
    for far in range(1, groups):
        order = jnp.array([block ^ far for block in range(groups)])
        shared = jnp.maximum(shared, lax.ppermute(peaks, "dp", flips(dp_count, far * square))[order])
    steps = power_steps(shared)

    def partial_sum(far):
        total = sum(
            quantize(raw[near][far], 1.0 / steps[far], codes[near][far]) for near in range(square)
        )
        return total.astype(jnp.bfloat16)

    place = lax.axis_index("expert")
    holder_of = [
        jnp.sum(jnp.where(slot_expert == (place ^ flip), jnp.arange(expert_count), 0))
        for flip in range(expert_count)
    ]
    own = partial_sum(0)
    beside = lax.ppermute(own, "expert", flips(expert_count, 1))
    across_wants = jnp.where(holder_of[2] == place, own, beside)
    across = lax.ppermute(across_wants, "expert", flips(expert_count, 2))
    mine = holder_of[0]
    near_sum = jnp.where(mine == place, own, jnp.where(mine == (place ^ 1), beside, across))

    step_rows = jnp.broadcast_to(steps[1].astype(jnp.bfloat16), (8, hidden))
    message = jnp.concatenate([partial_sum(1), step_rows])
    orders = list(itertools.permutations(range(expert_count)))
    match = [
        jnp.all(slot_expert == jnp.array(order, jnp.int32)).astype(jnp.int32) * number
        for number, order in enumerate(orders)
    ]

    def route(order):
        pairs = [
            (block * expert_count + slot, (block ^ square) * expert_count + order[slot])
            for block in range(dp_count)
            for slot in range(expert_count)
        ]
        return lambda parts: lax.ppermute(parts, ("dp", "expert"), pairs)

    arrived = lax.switch(sum(match), [route(order) for order in orders], message)
    totals = near_sum.astype(jnp.float32) + arrived[:block_rows].astype(jnp.float32)
    step = arrived[block_rows, 0].astype(jnp.float32)
    mean_grad, new_weight = apply_update((totals * (step / dp_count))[None], master_weight)
    return mean_grad, new_weight, step.reshape(1, 1)


def solution(mesh):
    dp_count, expert_count = mesh.shape["dp"], mesh.shape["expert"]

    def body(expert_grads, round_offsets, slot_expert, master_weight):
        staged = (
            dp_count == 2 * square
            and expert_count == 4
            and expert_grads.shape[1] == 1
            and expert_grads.shape[2] % (8 * dp_count) == 0
        )
        chosen = staged_body if staged else general_body
        return chosen(expert_grads, round_offsets, slot_expert, master_weight)

    return jax.shard_map(
        body,
        mesh=mesh,
        in_specs=(
            P("dp", "expert", None, None),
            P("dp", "expert", None),
            P(),
            P("expert", "dp", None),
        ),
        out_specs=(P("expert", "dp", None), P("expert", "dp", None), P("expert", "dp")),
        check_vma=False,
    )
```

```python
import functools
import itertools

import jax
import jax.numpy as jnp
from jax import lax
from jax.experimental import pallas as pl
from jax.experimental.pallas import tpu as pltpu
from jax.sharding import PartitionSpec as P

level_bits = 6
low_power = -30
high_power = 30
learn_rate = 0.05
field_base = 32768
count_shift = 64
square = 4


def power_steps(maxima):
    powers = jnp.array([2.0**exponent for exponent in range(low_power, high_power)], jnp.float32)
    reached = maxima[..., None] >= powers
    doubled = jnp.prod(jnp.where(reached, jnp.float32(2.0), jnp.float32(1.0)), axis=-1)
    return 2.0 ** (low_power - level_bits) * doubled


def dither(element_code):
    mixed = element_code * 747796405 + 1013904223
    mixed = jnp.bitwise_xor(mixed, jnp.right_shift(mixed, 13))
    mixed = mixed * 1103515245
    mixed = jnp.bitwise_xor(mixed, jnp.right_shift(mixed, 16))
    return jnp.bitwise_and(jnp.right_shift(mixed, 12), 255).astype(jnp.float32) / 256.0


def quantize(values, inverse_step, offsets):
    columns = lax.broadcasted_iota(jnp.int32, (1, values.shape[-1]), 1)
    element_code = offsets[..., None] + columns
    scaled = values.astype(jnp.float32) * inverse_step
    floor_part = jnp.floor(scaled)
    return floor_part + jnp.floor(scaled - floor_part + dither(element_code))


def apply_update(mean_grad, master_weight):
    return mean_grad, master_weight - learn_rate * mean_grad


def general_body(expert_grads, round_offsets, slot_expert, master_weight):
    dp_count = lax.axis_size("dp")
    local_grads = expert_grads[0]
    slot_count, row_count, hidden = local_grads.shape
    block_rows = row_count // dp_count
    shaped = local_grads.reshape(slot_count, dp_count, block_rows, hidden)
    maxima = lax.pmax(jnp.max(jnp.abs(shaped), axis=(2, 3)).astype(jnp.float32), "dp")
    all_steps = power_steps(maxima)
    counts = quantize(
        shaped,
        (1.0 / all_steps)[:, :, None, None],
        round_offsets[0].reshape(slot_count, dp_count, block_rows),
    ).astype(jnp.int32).reshape(slot_count, row_count, hidden)
    half = hidden // 2
    words = (counts[:, :, :half] + count_shift) * field_base + (counts[:, :, half:] + count_shift)
    summed = lax.psum_scatter(words, "dp", scatter_dimension=1, tiled=True)
    upper = jnp.right_shift(summed, 15) - count_shift * dp_count
    lower = jnp.bitwise_and(summed, field_base - 1) - count_shift * dp_count
    totals = jnp.concatenate([upper, lower], axis=2)
    step_sizes = lax.dynamic_slice_in_dim(all_steps, lax.axis_index("dp"), 1, 1)
    mean_slot = totals.astype(jnp.float32) * (step_sizes / dp_count)[..., None]
    gathered = lax.all_gather(mean_slot, "expert", axis=0, tiled=True)
    gathered_steps = lax.all_gather(step_sizes, "expert", axis=0, tiled=True)
    wanted = lax.axis_index("expert") * slot_count + lax.broadcasted_iota(
        jnp.int32, (slot_count, 1), 0
    )
    positions = lax.broadcasted_iota(jnp.int32, (1, slot_expert.shape[0]), 1)
    holder = jnp.sum(jnp.where(slot_expert[None, :] == wanted, positions, 0), axis=1)
    mean_grad, new_weight = apply_update(gathered[holder], master_weight)
    return mean_grad, new_weight, gathered_steps[holder]


def flips(count, mask):
    return [(index, index ^ mask) for index in range(count)]


def power_of_two(exponent):
    result = jnp.ones(exponent.shape, jnp.float32)
    size = jnp.abs(exponent)
    for bit in range(6):
        factor = jnp.where(exponent < 0, jnp.float32(2.0 ** -(2**bit)), jnp.float32(2.0 ** (2**bit)))
        result = result * jnp.where((size >> bit) & 1 == 1, factor, jnp.float32(1.0))
    return result


def sum_kernel(far, rows, *refs):
    notes, raws, out, codes = refs[:square], refs[square : 2 * square], refs[-2], refs[-1]
    target = lax.axis_index("dp") ^ (far * square)
    counts = notes[0][2:3, :]
    for note in notes[1:]:
        counts = jnp.maximum(counts, note[2:3, :])
    lanes = lax.broadcasted_iota(jnp.int32, counts.shape, 1)
    reached = jnp.where(lanes == target, counts, 0).astype(jnp.float32)
    exponent = jnp.max(reached, axis=1, keepdims=True).astype(jnp.int32) + (low_power - level_bits)
    inverse_step = power_of_two(-exponent)
    seeds = jnp.concatenate([note[far : far + 1, :] for note in notes] * 2)
    codes[...] = jnp.transpose(seeds) * 747796405 + 1013904223
    height, width = 16, raws[0].shape[1]
    columns = lax.broadcasted_iota(jnp.int32, (1, width), 1) * 747796405

    def step(index, carry):
        span = pl.ds(pl.multiple_of(index * height, height), height)
        total = jnp.zeros((height, width), jnp.float32)
        for near in range(square):
            mixed = codes[span, near : near + 1] + columns
            mixed = jnp.bitwise_xor(mixed, jnp.right_shift(mixed, 13))
            mixed = mixed * 1103515245
            mixed = jnp.bitwise_xor(mixed, jnp.right_shift(mixed, 16))
            noise = jnp.bitwise_and(jnp.right_shift(mixed, 12), 255).astype(jnp.float32) * (1.0 / 256.0)
            scaled = raws[near][span, :].astype(jnp.float32) * inverse_step
            floor_part = jnp.floor(scaled)
            total = total + (floor_part + jnp.floor(scaled - floor_part + noise))
        out[span, :] = total.astype(jnp.bfloat16)
        return carry

    lax.fori_loop(0, rows // height, step, 0)
    if out.shape[0] > rows:
        tail = (out.shape[0] - rows, width)
        out[rows:, :] = jnp.broadcast_to(power_of_two(exponent), tail).astype(jnp.bfloat16)


def sum_counts(far, notes, raws, extra):
    rows, width = raws[0].shape
    whole = pl.BlockSpec(memory_space=pltpu.VMEM)
    return pl.pallas_call(
        functools.partial(sum_kernel, far, rows),
        out_shape=jax.ShapeDtypeStruct((rows + extra, width), jnp.bfloat16),
        in_specs=[whole] * (2 * square),
        out_specs=whole,
        scratch_shapes=[pltpu.VMEM((rows, 2 * square), jnp.int32)],
        cost_estimate=pl.CostEstimate(
            flops=20 * square * rows * width,
            bytes_accessed=2 * (square + 1) * rows * width,
            transcendentals=0,
        ),
        compiler_params=pltpu.CompilerParams(vmem_limit_bytes=8 * 2**20),
        name="sum_far" if far else "sum_near",
    )(*notes, *raws)


def staged_body(expert_grads, round_offsets, slot_expert, master_weight):
    dp_count = lax.axis_size("dp")
    expert_count = lax.axis_size("expert")
    row_count, hidden = expert_grads.shape[2:]
    block_rows = row_count // dp_count
    me = lax.axis_index("dp")
    place = lax.axis_index("expert")
    blocks = expert_grads[0, 0].reshape(dp_count, block_rows, hidden)
    offsets = round_offsets[0, 0].reshape(dp_count, block_rows)

    def pick(array, index):
        return lax.dynamic_index_in_dim(array, index, 0, keepdims=False)

    after = jnp.arange(expert_count)[None, :] > jnp.arange(expert_count)[:, None]
    weights = jnp.array([6, 2, 1, 0], jnp.int32)[:, None]
    lower = (slot_expert[:, None] > slot_expert[None, :]) & after
    branch = jnp.sum(jnp.where(lower, weights, 0))
    peaks = jnp.max(jnp.abs(blocks), axis=(1, 2)).astype(jnp.float32)
    twin = lax.ppermute(peaks, "dp", flips(dp_count, square))
    powers = jnp.array([2.0**power for power in range(low_power, high_power)], jnp.float32)
    reached = jnp.maximum(peaks, twin)[:, None] >= powers
    counts = jnp.sum(reached.astype(jnp.int32), axis=1)
    counts = jnp.pad(counts, (0, block_rows - dp_count))

    raw, notes = [[], []], []
    for near in range(square):
        picked = [(me ^ near) ^ (far * square) for far in range(2)]
        seeds = [pick(offsets, target) for target in picked]
        note = jnp.concatenate([jnp.stack(seeds + [counts]), jnp.zeros((5, block_rows), jnp.int32)])
        rows = [pick(blocks, target) for target in picked]
        if near:
            pairs = flips(dp_count, near)
            note = lax.ppermute(note, "dp", pairs)
            for far in range(2):
                rows[far] = lax.ppermute(rows[far], "dp", pairs)
        notes.append(note)
        for far in range(2):
            raw[far].append(rows[far])

    holder_of = [
        jnp.sum(jnp.where(slot_expert == (place ^ flip), jnp.arange(expert_count), 0))
        for flip in range(expert_count)
    ]
    own = sum_counts(0, notes, raw[0], 0)
    beside = lax.ppermute(own, "expert", flips(expert_count, 1))
    across_wants = jnp.where(holder_of[2] == place, own, beside)
    across = lax.ppermute(across_wants, "expert", flips(expert_count, 2))
    message = sum_counts(1, notes, raw[1], 8)

    def route(order):
        pairs = [
            (block * expert_count + slot, (block ^ square) * expert_count + order[slot])
            for block in range(dp_count)
            for slot in range(expert_count)
        ]
        return lambda parts: lax.ppermute(parts, ("dp", "expert"), pairs)

    orders = itertools.permutations(range(expert_count))
    arrived = lax.switch(branch, [route(order) for order in orders], message)
    mine = holder_of[0]
    near_sum = jnp.where(mine == place, own, jnp.where(mine == (place ^ 1), beside, across))
    totals = near_sum.astype(jnp.float32) + arrived[:block_rows].astype(jnp.float32)
    step = arrived[block_rows, 0].astype(jnp.float32)
    mean_grad, new_weight = apply_update((totals * (step / dp_count))[None], master_weight)
    return mean_grad, new_weight, step.reshape(1, 1)


def solution(mesh):
    staged = mesh.shape["dp"] == 2 * square and mesh.shape["expert"] == 4
    return jax.shard_map(
        staged_body if staged else general_body,
        mesh=mesh,
        in_specs=(
            P("dp", "expert", None, None),
            P("dp", "expert", None),
            P(),
            P("expert", "dp", None),
        ),
        out_specs=(P("expert", "dp", None), P("expert", "dp", None), P("expert", "dp")),
        check_vma=False,
    )
```

```python
import functools
import itertools

import jax
import jax.numpy as jnp
from jax import lax
from jax.experimental import pallas as pl
from jax.experimental.pallas import tpu as pltpu
from jax.sharding import PartitionSpec as P

level_bits = 6
low_power = -30
high_power = 30
learn_rate = 0.05
field_base = 32768
count_shift = 64
square = 4


def power_steps(maxima):
    powers = jnp.array([2.0**exponent for exponent in range(low_power, high_power)], jnp.float32)
    reached = maxima[..., None] >= powers
    doubled = jnp.prod(jnp.where(reached, jnp.float32(2.0), jnp.float32(1.0)), axis=-1)
    return 2.0 ** (low_power - level_bits) * doubled


def dither(element_code):
    mixed = element_code * 747796405 + 1013904223
    mixed = jnp.bitwise_xor(mixed, jnp.right_shift(mixed, 13))
    mixed = mixed * 1103515245
    mixed = jnp.bitwise_xor(mixed, jnp.right_shift(mixed, 16))
    return jnp.bitwise_and(jnp.right_shift(mixed, 12), 255).astype(jnp.float32) / 256.0


def quantize(values, inverse_step, offsets):
    columns = lax.broadcasted_iota(jnp.int32, (1, values.shape[-1]), 1)
    element_code = offsets[..., None] + columns
    scaled = values.astype(jnp.float32) * inverse_step
    floor_part = jnp.floor(scaled)
    return floor_part + jnp.floor(scaled - floor_part + dither(element_code))


def apply_update(mean_grad, master_weight):
    return mean_grad, master_weight - learn_rate * mean_grad


def general_body(expert_grads, round_offsets, slot_expert, master_weight):
    dp_count = lax.axis_size("dp")
    local_grads = expert_grads[0]
    slot_count, row_count, hidden = local_grads.shape
    block_rows = row_count // dp_count
    shaped = local_grads.reshape(slot_count, dp_count, block_rows, hidden)
    maxima = lax.pmax(jnp.max(jnp.abs(shaped), axis=(2, 3)).astype(jnp.float32), "dp")
    all_steps = power_steps(maxima)
    counts = quantize(
        shaped,
        (1.0 / all_steps)[:, :, None, None],
        round_offsets[0].reshape(slot_count, dp_count, block_rows),
    ).astype(jnp.int32).reshape(slot_count, row_count, hidden)
    half = hidden // 2
    words = (counts[:, :, :half] + count_shift) * field_base + (counts[:, :, half:] + count_shift)
    summed = lax.psum_scatter(words, "dp", scatter_dimension=1, tiled=True)
    upper = jnp.right_shift(summed, 15) - count_shift * dp_count
    lower = jnp.bitwise_and(summed, field_base - 1) - count_shift * dp_count
    totals = jnp.concatenate([upper, lower], axis=2)
    step_sizes = lax.dynamic_slice_in_dim(all_steps, lax.axis_index("dp"), 1, 1)
    mean_slot = totals.astype(jnp.float32) * (step_sizes / dp_count)[..., None]
    gathered = lax.all_gather(mean_slot, "expert", axis=0, tiled=True)
    gathered_steps = lax.all_gather(step_sizes, "expert", axis=0, tiled=True)
    wanted = lax.axis_index("expert") * slot_count + lax.broadcasted_iota(
        jnp.int32, (slot_count, 1), 0
    )
    positions = lax.broadcasted_iota(jnp.int32, (1, slot_expert.shape[0]), 1)
    holder = jnp.sum(jnp.where(slot_expert[None, :] == wanted, positions, 0), axis=1)
    mean_grad, new_weight = apply_update(gathered[holder], master_weight)
    return mean_grad, new_weight, gathered_steps[holder]


def flips(count, mask):
    return [(index, index ^ mask) for index in range(count)]


def power_of_two(exponent):
    result = jnp.ones(exponent.shape, jnp.float32)
    size = jnp.abs(exponent)
    for bit in range(6):
        factor = jnp.where(exponent < 0, jnp.float32(2.0 ** -(2**bit)), jnp.float32(2.0 ** (2**bit)))
        result = result * jnp.where((size >> bit) & 1 == 1, factor, jnp.float32(1.0))
    return result


def sum_kernel(far, rows, *refs):
    notes, raws, out, codes = refs[:square], refs[square : 2 * square], refs[-2], refs[-1]
    target = lax.axis_index("dp") ^ (far * square)
    counts = notes[0][2:3, :]
    for note in notes[1:]:
        counts = jnp.maximum(counts, note[2:3, :])
    lanes = lax.broadcasted_iota(jnp.int32, counts.shape, 1)
    reached = jnp.where(lanes == target, counts, 0).astype(jnp.float32)
    exponent = jnp.max(reached, axis=1, keepdims=True).astype(jnp.int32) + (low_power - level_bits)
    inverse_step = power_of_two(-exponent)
    seeds = jnp.concatenate([note[far : far + 1, :] for note in notes] * 2)
    codes[...] = jnp.transpose(seeds) * 747796405 + 1013904223
    height, width = 16, raws[0].shape[1]
    columns = lax.broadcasted_iota(jnp.int32, (1, width), 1) * 747796405

    def step(index, carry):
        span = pl.ds(pl.multiple_of(index * height, height), height)
        total = jnp.zeros((height, width), jnp.float32)
        for near in range(square):
            mixed = codes[span, near : near + 1] + columns
            mixed = jnp.bitwise_xor(mixed, jnp.right_shift(mixed, 13))
            mixed = mixed * 1103515245
            mixed = jnp.bitwise_xor(mixed, jnp.right_shift(mixed, 16))
            noise = jnp.bitwise_and(jnp.right_shift(mixed, 12), 255).astype(jnp.float32) * (1.0 / 256.0)
            scaled = raws[near][span, :].astype(jnp.float32) * inverse_step
            floor_part = jnp.floor(scaled)
            total = total + (floor_part + jnp.floor(scaled - floor_part + noise))
        out[span, :] = total.astype(jnp.bfloat16)
        return carry

    lax.fori_loop(0, rows // height, step, 0)
    if out.shape[0] > rows:
        tail = (out.shape[0] - rows, width)
        out[rows:, :] = jnp.broadcast_to(power_of_two(exponent), tail).astype(jnp.bfloat16)


def sum_counts(far, notes, raws, extra):
    rows, width = raws[0].shape
    whole = pl.BlockSpec(memory_space=pltpu.VMEM)
    return pl.pallas_call(
        functools.partial(sum_kernel, far, rows),
        out_shape=jax.ShapeDtypeStruct((rows + extra, width), jnp.bfloat16),
        in_specs=[whole] * (2 * square),
        out_specs=whole,
        scratch_shapes=[pltpu.VMEM((rows, 2 * square), jnp.int32)],
        cost_estimate=pl.CostEstimate(
            flops=20 * square * rows * width,
            bytes_accessed=2 * (square + 1) * rows * width,
            transcendentals=0,
        ),
        compiler_params=pltpu.CompilerParams(vmem_limit_bytes=8 * 2**20),
        name="sum_far" if far else "sum_near",
    )(*notes, *raws)


def update_kernel(dp_count, slots, own, beside, across, arrived, weight, mean, updated, step):
    index = pl.program_id(0)
    place = lax.axis_index("expert")
    holder = jnp.int32(0)
    for slot in range(slots.shape[0]):
        holder = jnp.where(slots[slot] == place, slot, holder)
    turn = holder ^ place
    rows = mean.shape[1]
    span = pl.ds(pl.multiple_of(index * rows, rows), rows)
    last = own.shape[0] - arrived.shape[0]
    tail = pl.ds(arrived.shape[0], last)

    def nearby(where):
        held, swapped, crossed = (ref[where, :].astype(jnp.float32) for ref in (own, beside, across))
        return jnp.where(turn == 0, held, jnp.where(turn == 1, swapped, crossed))

    size = nearby(tail)[0:1, :]
    total = nearby(span) + arrived[span, :].astype(jnp.float32)
    averaged = total * (size * (1.0 / dp_count))
    mean[0] = averaged
    updated[0] = weight[0] - learn_rate * averaged
    step[...] = size[:, 0:1]


def update(slots, own, beside, across, arrived, weight, dp_count):
    rows, width = arrived.shape
    parts = 4
    whole = pl.BlockSpec(memory_space=pltpu.VMEM)
    strip = pl.BlockSpec((1, rows // parts, width), lambda index: (0, index, 0))
    block = jax.ShapeDtypeStruct((1, rows, width), jnp.float32)
    return pl.pallas_call(
        functools.partial(update_kernel, dp_count),
        grid=(parts,),
        out_shape=(block, block, jax.ShapeDtypeStruct((1, 1), jnp.float32)),
        in_specs=[pl.BlockSpec(memory_space=pltpu.SMEM), whole, whole, whole, whole, strip],
        out_specs=(strip, strip, pl.BlockSpec((1, 1), lambda index: (0, 0))),
        compiler_params=pltpu.CompilerParams(vmem_limit_bytes=8 * 2**20),
        name="update",
    )(slots, own, beside, across, arrived, weight)


def staged_body(expert_grads, round_offsets, slot_expert, master_weight):
    dp_count = lax.axis_size("dp")
    expert_count = lax.axis_size("expert")
    row_count, hidden = expert_grads.shape[2:]
    block_rows = row_count // dp_count
    me = lax.axis_index("dp")
    place = lax.axis_index("expert")
    blocks = expert_grads[0, 0].reshape(dp_count, block_rows, hidden)
    offsets = round_offsets[0, 0].reshape(dp_count, block_rows)

    def pick(array, index):
        return lax.dynamic_index_in_dim(array, index, 0, keepdims=False)

    after = jnp.arange(expert_count)[None, :] > jnp.arange(expert_count)[:, None]
    weights = jnp.array([6, 2, 1, 0], jnp.int32)[:, None]
    lower = (slot_expert[:, None] > slot_expert[None, :]) & after
    branch = jnp.sum(jnp.where(lower, weights, 0))
    peaks = jnp.max(jnp.abs(blocks), axis=(1, 2)).astype(jnp.float32)
    twin = lax.ppermute(peaks, "dp", flips(dp_count, square))
    powers = jnp.array([2.0**power for power in range(low_power, high_power)], jnp.float32)
    reached = jnp.maximum(peaks, twin)[:, None] >= powers
    counts = jnp.sum(reached.astype(jnp.int32), axis=1)
    counts = jnp.pad(counts, (0, block_rows - dp_count))

    later = lax.optimization_barrier(blocks)
    raw, notes = [[], []], []
    for near in range(square):
        targets = [(me ^ near) ^ (far * square) for far in range(2)]
        seeds = [pick(offsets, target) for target in targets]
        note = jnp.concatenate([jnp.stack(seeds + [counts]), jnp.zeros((5, block_rows), jnp.int32)])
        rows = [pick(blocks if near else later, targets[0]), pick(later, targets[1])]
        if near:
            pairs = flips(dp_count, near)
            note = lax.ppermute(note, "dp", pairs)
            for far in range(2):
                rows[far] = lax.ppermute(rows[far], "dp", pairs)
        notes.append(note)
        for far in range(2):
            raw[far].append(rows[far])

    wanted = slot_expert == (place ^ 2)
    holder = jnp.sum(jnp.where(wanted, jnp.arange(expert_count), 0))
    own = sum_counts(0, notes, raw[0], 8)
    beside = lax.ppermute(own, "expert", flips(expert_count, 1))
    across_wants = jnp.where(holder == place, own, beside)
    across = lax.ppermute(across_wants, "expert", flips(expert_count, 2))
    message = sum_counts(1, notes, raw[1], 0)

    def route(order):
        pairs = [
            (block * expert_count + slot, (block ^ square) * expert_count + order[slot])
            for block in range(dp_count)
            for slot in range(expert_count)
        ]
        return lambda parts: lax.ppermute(parts, ("dp", "expert"), pairs)

    orders = itertools.permutations(range(expert_count))
    arrived = lax.switch(branch, [route(order) for order in orders], message)
    return update(slot_expert, own, beside, across, arrived, master_weight, dp_count)


def solution(mesh):
    staged = mesh.shape["dp"] == 2 * square and mesh.shape["expert"] == 4
    return jax.shard_map(
        staged_body if staged else general_body,
        mesh=mesh,
        in_specs=(
            P("dp", "expert", None, None),
            P("dp", "expert", None),
            P(),
            P("expert", "dp", None),
        ),
        out_specs=(P("expert", "dp", None), P("expert", "dp", None), P("expert", "dp")),
        check_vma=False,
    )
```

```python
import functools
import itertools

import jax
import jax.numpy as jnp
from jax import lax
from jax.experimental import pallas as pl
from jax.experimental.pallas import tpu as pltpu
from jax.sharding import PartitionSpec as P

level_bits = 6
low_power = -30
high_power = 30
learn_rate = 0.05
field_base = 32768
count_shift = 64
square = 4


def power_steps(maxima):
    powers = jnp.array([2.0**exponent for exponent in range(low_power, high_power)], jnp.float32)
    reached = maxima[..., None] >= powers
    doubled = jnp.prod(jnp.where(reached, jnp.float32(2.0), jnp.float32(1.0)), axis=-1)
    return 2.0 ** (low_power - level_bits) * doubled


def dither(element_code):
    mixed = element_code * 747796405 + 1013904223
    mixed = jnp.bitwise_xor(mixed, jnp.right_shift(mixed, 13))
    mixed = mixed * 1103515245
    mixed = jnp.bitwise_xor(mixed, jnp.right_shift(mixed, 16))
    return jnp.bitwise_and(jnp.right_shift(mixed, 12), 255).astype(jnp.float32) / 256.0


def quantize(values, inverse_step, offsets):
    columns = lax.broadcasted_iota(jnp.int32, (1, values.shape[-1]), 1)
    element_code = offsets[..., None] + columns
    scaled = values.astype(jnp.float32) * inverse_step
    floor_part = jnp.floor(scaled)
    return floor_part + jnp.floor(scaled - floor_part + dither(element_code))


def apply_update(mean_grad, master_weight):
    return mean_grad, master_weight - learn_rate * mean_grad


def general_body(expert_grads, round_offsets, slot_expert, master_weight):
    dp_count = lax.axis_size("dp")
    local_grads = expert_grads[0]
    slot_count, row_count, hidden = local_grads.shape
    block_rows = row_count // dp_count
    shaped = local_grads.reshape(slot_count, dp_count, block_rows, hidden)
    maxima = lax.pmax(jnp.max(jnp.abs(shaped), axis=(2, 3)).astype(jnp.float32), "dp")
    all_steps = power_steps(maxima)
    counts = quantize(
        shaped,
        (1.0 / all_steps)[:, :, None, None],
        round_offsets[0].reshape(slot_count, dp_count, block_rows),
    ).astype(jnp.int32).reshape(slot_count, row_count, hidden)
    half = hidden // 2
    words = (counts[:, :, :half] + count_shift) * field_base + (counts[:, :, half:] + count_shift)
    summed = lax.psum_scatter(words, "dp", scatter_dimension=1, tiled=True)
    upper = jnp.right_shift(summed, 15) - count_shift * dp_count
    lower = jnp.bitwise_and(summed, field_base - 1) - count_shift * dp_count
    totals = jnp.concatenate([upper, lower], axis=2)
    step_sizes = lax.dynamic_slice_in_dim(all_steps, lax.axis_index("dp"), 1, 1)
    mean_slot = totals.astype(jnp.float32) * (step_sizes / dp_count)[..., None]
    gathered = lax.all_gather(mean_slot, "expert", axis=0, tiled=True)
    gathered_steps = lax.all_gather(step_sizes, "expert", axis=0, tiled=True)
    wanted = lax.axis_index("expert") * slot_count + lax.broadcasted_iota(
        jnp.int32, (slot_count, 1), 0
    )
    positions = lax.broadcasted_iota(jnp.int32, (1, slot_expert.shape[0]), 1)
    holder = jnp.sum(jnp.where(slot_expert[None, :] == wanted, positions, 0), axis=1)
    mean_grad, new_weight = apply_update(gathered[holder], master_weight)
    return mean_grad, new_weight, gathered_steps[holder]


def flips(count, mask):
    return [(index, index ^ mask) for index in range(count)]


def power_of_two(exponent):
    result = jnp.ones(exponent.shape, jnp.float32)
    size = jnp.abs(exponent)
    for bit in range(6):
        factor = jnp.where(exponent < 0, jnp.float32(2.0 ** -(2**bit)), jnp.float32(2.0 ** (2**bit)))
        result = result * jnp.where((size >> bit) & 1 == 1, factor, jnp.float32(1.0))
    return result


def block_at(grads, target, rows):
    return grads.at[0, 0, pl.ds(pl.multiple_of(target * rows, rows), rows), :]


def largest(ref):
    height = 16
    best = jnp.abs(ref[0:height, :])
    for row in range(height, ref.shape[0], height):
        best = jnp.maximum(best, jnp.abs(ref[row : row + height, :]))
    best = jnp.max(best.astype(jnp.float32), axis=0, keepdims=True)
    return jnp.max(best, axis=1, keepdims=True)


def first_kernel(grads, *refs):
    outs, sems = refs[:-1], refs[-1]
    me = lax.axis_index("dp")
    copies = []
    for near in range(1, square):
        out = outs[near - 1]
        copy = pltpu.make_async_copy(block_at(grads, me ^ near, out.shape[0]), out, sems.at[near - 1])
        copy.start()
        copies.append(copy)
    for copy in copies:
        copy.wait()


def second_kernel(grads, *refs):
    given, outs, levels, sems = refs[: square - 1], refs[square - 1 : -2], refs[-2], refs[-1]
    me = lax.axis_index("dp")
    targets = [me] + [me ^ square ^ near for near in range(square)]
    copies = []
    for number, target in enumerate(targets):
        out = outs[number]
        copy = pltpu.make_async_copy(block_at(grads, target, out.shape[0]), out, sems.at[number])
        copy.start()
        copies.append(copy)
    lanes = lax.broadcasted_iota(jnp.int32, levels.shape, 1)
    peaks = jnp.zeros(levels.shape, jnp.float32)
    for near in range(1, square):
        peaks = jnp.where(lanes == (me ^ near), largest(given[near - 1]), peaks)
    for number, target in enumerate(targets):
        copies[number].wait()
        peaks = jnp.where(lanes == target, largest(outs[number]), peaks)
    counts = [jnp.zeros(levels.shape, jnp.int32) for _ in range(4)]
    for power in range(low_power, high_power):
        counts[power % 4] += (peaks >= jnp.float32(2.0**power)).astype(jnp.int32)
    levels[...] = (counts[0] + counts[1]) + (counts[2] + counts[3])


def pack(grads, rows, given):
    width = grads.shape[-1]
    vmem = pl.BlockSpec(memory_space=pltpu.VMEM)
    block = jax.ShapeDtypeStruct((rows, width), grads.dtype)
    count = square + 1 if given else square - 1
    levels = [jax.ShapeDtypeStruct((8, rows), jnp.int32)] if given else []
    return pl.pallas_call(
        second_kernel if given else first_kernel,
        out_shape=[block] * count + levels,
        in_specs=[pl.BlockSpec(memory_space=pltpu.HBM)] + [vmem] * len(given),
        out_specs=[vmem] * (count + len(levels)),
        scratch_shapes=[pltpu.SemaphoreType.DMA((count,))],
        compiler_params=pltpu.CompilerParams(vmem_limit_bytes=8 * 2**20),
        name="pack_rest" if given else "pack_own",
    )(pltpu.with_memory_space_constraint(grads, pltpu.HBM), *given)


def noise_of(codes, columns):
    mixed = codes + columns
    mixed = jnp.bitwise_xor(mixed, jnp.right_shift(mixed, 13))
    mixed = mixed * 1103515245
    mixed = jnp.bitwise_xor(mixed, jnp.right_shift(mixed, 16))
    return jnp.bitwise_and(jnp.right_shift(mixed, 12), 255).astype(jnp.float32) * (1.0 / 256.0)


def fill_codes(far, notes, codes):
    seeds = jnp.concatenate([note[far : far + 1, :] for note in notes] * 2)
    codes[...] = jnp.transpose(seeds) * 747796405 + 1013904223


def noise_kernel(far, *refs):
    notes, out, codes = refs[:square], refs[square], refs[square + 1]
    fill_codes(far, notes, codes)
    height, width = 16, out.shape[2]
    columns = lax.broadcasted_iota(jnp.int32, (1, width), 1) * 747796405

    def step(index, carry):
        span = pl.ds(pl.multiple_of(index * height, height), height)
        for near in range(square):
            out[near, span, :] = noise_of(codes[span, near : near + 1], columns).astype(jnp.bfloat16)
        return carry

    lax.fori_loop(0, out.shape[1] // height, step, 0)


def make_noise(far, notes, rows, width):
    vmem = pl.BlockSpec(memory_space=pltpu.VMEM)
    return pl.pallas_call(
        functools.partial(noise_kernel, far),
        out_shape=jax.ShapeDtypeStruct((square, rows, width), jnp.bfloat16),
        in_specs=[vmem] * square,
        out_specs=vmem,
        scratch_shapes=[pltpu.VMEM((rows, 2 * square), jnp.int32)],
        compiler_params=pltpu.CompilerParams(vmem_limit_bytes=8 * 2**20),
        name="noise",
    )(*notes)


def sum_kernel(far, rows, *refs):
    notes, raws, rest = refs[:square], refs[square : 2 * square], refs[2 * square :]
    noise, out, codes = (None, *rest) if far == 0 else (*rest, None)
    target = lax.axis_index("dp") ^ (far * square)
    counts = notes[0][2:3, :]
    for note in notes[1:]:
        counts = jnp.maximum(counts, note[2:3, :])
    lanes = lax.broadcasted_iota(jnp.int32, counts.shape, 1)
    reached = jnp.where(lanes == target, counts, 0).astype(jnp.float32)
    exponent = jnp.max(reached, axis=1, keepdims=True).astype(jnp.int32) + (low_power - level_bits)
    inverse_step = power_of_two(-exponent)
    height, width = 16, raws[0].shape[1]
    columns = lax.broadcasted_iota(jnp.int32, (1, width), 1) * 747796405
    if noise is None:
        fill_codes(far, notes, codes)

    def step(index, carry):
        span = pl.ds(pl.multiple_of(index * height, height), height)
        total = jnp.zeros((height, width), jnp.float32)
        for near in range(square):
            if noise is None:
                drawn = noise_of(codes[span, near : near + 1], columns)
            else:
                drawn = noise[near, span, :].astype(jnp.float32)
            scaled = raws[near][span, :].astype(jnp.float32) * inverse_step
            floor_part = jnp.floor(scaled)
            total = total + (floor_part + jnp.floor(scaled - floor_part + drawn))
        out[span, :] = total.astype(jnp.bfloat16)
        return carry

    lax.fori_loop(0, rows // height, step, 0)
    if out.shape[0] > rows:
        tail = (out.shape[0] - rows, width)
        out[rows:, :] = jnp.broadcast_to(power_of_two(exponent), tail).astype(jnp.bfloat16)


def sum_counts(far, notes, raws, noise, extra):
    rows, width = raws[0].shape
    vmem = pl.BlockSpec(memory_space=pltpu.VMEM)
    more = [noise] if far else []
    return pl.pallas_call(
        functools.partial(sum_kernel, far, rows),
        out_shape=jax.ShapeDtypeStruct((rows + extra, width), jnp.bfloat16),
        in_specs=[vmem] * (2 * square + len(more)),
        out_specs=vmem,
        scratch_shapes=[] if far else [pltpu.VMEM((rows, 2 * square), jnp.int32)],
        compiler_params=pltpu.CompilerParams(vmem_limit_bytes=8 * 2**20),
        name="sum_far" if far else "sum_near",
    )(*notes, *raws, *more)


def update_kernel(dp_count, slots, own, beside, across, arrived, weight, *refs):
    mean, updated, step, means, news, sems = refs
    place = lax.axis_index("expert")
    holder = jnp.int32(0)
    for slot in range(slots.shape[0]):
        holder = jnp.where(slots[slot] == place, slot, holder)
    turn = holder ^ place
    rows = arrived.shape[0]

    def nearby(span):
        held, swapped, crossed = (ref[span, :].astype(jnp.float32) for ref in (own, beside, across))
        return jnp.where(turn == 0, held, jnp.where(turn == 1, swapped, crossed))

    size = nearby(slice(rows, own.shape[0]))[0:1, :]
    step[...] = size[:, 0:1]
    scale = size * (1.0 / dp_count)
    parts = sems.shape[1]
    height = rows // parts
    copies = []
    for part in range(parts):
        span = slice(part * height, (part + 1) * height)
        averaged = (nearby(span) + arrived[span, :].astype(jnp.float32)) * scale
        means[span, :] = averaged
        news[span, :] = weight[0, span, :] - learn_rate * averaged
        for number, (source, target) in enumerate(((means, mean), (news, updated))):
            copy = pltpu.make_async_copy(
                source.at[pl.ds(part * height, height), :],
                target.at[0, pl.ds(part * height, height), :],
                sems.at[number, part],
            )
            copy.start()
            copies.append(copy)
    for copy in copies:
        copy.wait()


def update(slots, own, beside, across, arrived, weight, dp_count):
    rows, width = arrived.shape
    parts = 4
    vmem = pl.BlockSpec(memory_space=pltpu.VMEM)
    hbm = pl.BlockSpec(memory_space=pltpu.HBM)
    block = jax.ShapeDtypeStruct((1, rows, width), jnp.float32)
    return pl.pallas_call(
        functools.partial(update_kernel, dp_count),
        out_shape=(block, block, jax.ShapeDtypeStruct((1, 1), jnp.float32)),
        in_specs=[pl.BlockSpec(memory_space=pltpu.SMEM)] + [vmem] * 5,
        out_specs=(hbm, hbm, vmem),
        scratch_shapes=[
            pltpu.VMEM((rows, width), jnp.float32),
            pltpu.VMEM((rows, width), jnp.float32),
            pltpu.SemaphoreType.DMA((2, parts)),
        ],
        compiler_params=pltpu.CompilerParams(vmem_limit_bytes=8 * 2**20),
        name="update",
    )(slots, own, beside, across, arrived, weight)


def staged_body(expert_grads, round_offsets, slot_expert, master_weight):
    dp_count = lax.axis_size("dp")
    expert_count = lax.axis_size("expert")
    row_count, hidden = expert_grads.shape[2:]
    block_rows = row_count // dp_count
    me = lax.axis_index("dp")
    place = lax.axis_index("expert")
    offsets = round_offsets[0, 0].reshape(dp_count, block_rows)

    def pick(array, index):
        return lax.dynamic_index_in_dim(array, index, 0, keepdims=False)

    after = jnp.arange(expert_count)[None, :] > jnp.arange(expert_count)[:, None]
    weights = jnp.array([6, 2, 1, 0], jnp.int32)[:, None]
    lower = (slot_expert[:, None] > slot_expert[None, :]) & after
    branch = jnp.sum(jnp.where(lower, weights, 0))
    near_blocks = pack(expert_grads, block_rows, [])
    *rest, levels = pack(expert_grads, block_rows, near_blocks)
    twin = lax.ppermute(levels, "dp", flips(dp_count, square))
    levels = jnp.maximum(levels[0], twin[0])

    raw, notes = [[rest[0], *near_blocks], rest[1:]], []
    for near in range(square):
        seeds = [pick(offsets, (me ^ near) ^ (far * square)) for far in range(2)]
        note = jnp.concatenate([jnp.stack(seeds + [levels]), jnp.zeros((5, block_rows), jnp.int32)])
        if near:
            pairs = flips(dp_count, near)
            note = lax.ppermute(note, "dp", pairs)
            for far in range(2):
                raw[far][near] = lax.ppermute(raw[far][near], "dp", pairs)
        notes.append(note)

    wanted = slot_expert == (place ^ 2)
    crossing = jnp.sum(jnp.where(wanted, jnp.arange(expert_count), 0)) == place
    own = sum_counts(0, notes, raw[0], None, 8)
    beside = lax.ppermute(own, "expert", flips(expert_count, 1))
    across_wants = jnp.where(crossing, own, beside)
    across = lax.ppermute(across_wants, "expert", flips(expert_count, 2))
    noise = make_noise(1, notes, block_rows, hidden)
    message = sum_counts(1, notes, raw[1], noise, 0)

    def route(order):
        pairs = [
            (block * expert_count + slot, (block ^ square) * expert_count + order[slot])
            for block in range(dp_count)
            for slot in range(expert_count)
        ]
        return lambda parts: lax.ppermute(parts, ("dp", "expert"), pairs)

    orders = itertools.permutations(range(expert_count))
    arrived = lax.switch(branch, [route(order) for order in orders], message)
    return update(slot_expert, own, beside, across, arrived, master_weight, dp_count)


def solution(mesh):
    staged = mesh.shape["dp"] == 2 * square and mesh.shape["expert"] == 4
    return jax.shard_map(
        staged_body if staged else general_body,
        mesh=mesh,
        in_specs=(
            P("dp", "expert", None, None),
            P("dp", "expert", None),
            P(),
            P("expert", "dp", None),
        ),
        out_specs=(P("expert", "dp", None), P("expert", "dp", None), P("expert", "dp")),
        check_vma=False,
    )
```

```python
import functools
import itertools

import jax
import jax.numpy as jnp
from jax import lax
from jax.experimental import pallas as pl
from jax.experimental.pallas import tpu as pltpu
from jax.sharding import PartitionSpec as P

level_bits = 6
low_power = -30
high_power = 30
learn_rate = 0.05
field_base = 32768
count_shift = 64
square = 4


def power_steps(maxima):
    powers = jnp.array([2.0**exponent for exponent in range(low_power, high_power)], jnp.float32)
    reached = maxima[..., None] >= powers
    doubled = jnp.prod(jnp.where(reached, jnp.float32(2.0), jnp.float32(1.0)), axis=-1)
    return 2.0 ** (low_power - level_bits) * doubled


def dither(element_code):
    mixed = element_code * 747796405 + 1013904223
    mixed = jnp.bitwise_xor(mixed, jnp.right_shift(mixed, 13))
    mixed = mixed * 1103515245
    mixed = jnp.bitwise_xor(mixed, jnp.right_shift(mixed, 16))
    return jnp.bitwise_and(jnp.right_shift(mixed, 12), 255).astype(jnp.float32) / 256.0


def quantize(values, inverse_step, offsets):
    columns = lax.broadcasted_iota(jnp.int32, (1, values.shape[-1]), 1)
    element_code = offsets[..., None] + columns
    scaled = values.astype(jnp.float32) * inverse_step
    floor_part = jnp.floor(scaled)
    return floor_part + jnp.floor(scaled - floor_part + dither(element_code))


def apply_update(mean_grad, master_weight):
    return mean_grad, master_weight - learn_rate * mean_grad


def general_body(expert_grads, round_offsets, slot_expert, master_weight):
    dp_count = lax.axis_size("dp")
    local_grads = expert_grads[0]
    slot_count, row_count, hidden = local_grads.shape
    block_rows = row_count // dp_count
    shaped = local_grads.reshape(slot_count, dp_count, block_rows, hidden)
    maxima = lax.pmax(jnp.max(jnp.abs(shaped), axis=(2, 3)).astype(jnp.float32), "dp")
    all_steps = power_steps(maxima)
    counts = quantize(
        shaped,
        (1.0 / all_steps)[:, :, None, None],
        round_offsets[0].reshape(slot_count, dp_count, block_rows),
    ).astype(jnp.int32).reshape(slot_count, row_count, hidden)
    half = hidden // 2
    words = (counts[:, :, :half] + count_shift) * field_base + (counts[:, :, half:] + count_shift)
    summed = lax.psum_scatter(words, "dp", scatter_dimension=1, tiled=True)
    upper = jnp.right_shift(summed, 15) - count_shift * dp_count
    lower = jnp.bitwise_and(summed, field_base - 1) - count_shift * dp_count
    totals = jnp.concatenate([upper, lower], axis=2)
    step_sizes = lax.dynamic_slice_in_dim(all_steps, lax.axis_index("dp"), 1, 1)
    mean_slot = totals.astype(jnp.float32) * (step_sizes / dp_count)[..., None]
    gathered = lax.all_gather(mean_slot, "expert", axis=0, tiled=True)
    gathered_steps = lax.all_gather(step_sizes, "expert", axis=0, tiled=True)
    wanted = lax.axis_index("expert") * slot_count + lax.broadcasted_iota(
        jnp.int32, (slot_count, 1), 0
    )
    positions = lax.broadcasted_iota(jnp.int32, (1, slot_expert.shape[0]), 1)
    holder = jnp.sum(jnp.where(slot_expert[None, :] == wanted, positions, 0), axis=1)
    mean_grad, new_weight = apply_update(gathered[holder], master_weight)
    return mean_grad, new_weight, gathered_steps[holder]


def flips(count, mask):
    return [(index, index ^ mask) for index in range(count)]


def power_of_two(exponent):
    result = jnp.ones(exponent.shape, jnp.float32)
    size = jnp.abs(exponent)
    for bit in range(6):
        factor = jnp.where(exponent < 0, jnp.float32(2.0 ** -(2**bit)), jnp.float32(2.0 ** (2**bit)))
        result = result * jnp.where((size >> bit) & 1 == 1, factor, jnp.float32(1.0))
    return result


def block_at(grads, target, rows):
    return grads.at[0, 0, pl.ds(pl.multiple_of(target * rows, rows), rows), :]


def largest(ref):
    height = 16
    best = jnp.abs(ref[0:height, :])
    for row in range(height, ref.shape[0], height):
        best = jnp.maximum(best, jnp.abs(ref[row : row + height, :]))
    best = jnp.max(best.astype(jnp.float32), axis=0, keepdims=True)
    return jnp.max(best, axis=1, keepdims=True)


def first_kernel(grads, *refs):
    outs, sems = refs[:-1], refs[-1]
    me = lax.axis_index("dp")
    copies = []
    for near in range(1, square):
        out = outs[near - 1]
        copy = pltpu.make_async_copy(block_at(grads, me ^ near, out.shape[0]), out, sems.at[near - 1])
        copy.start()
        copies.append(copy)
    for copy in copies:
        copy.wait()


def second_kernel(grads, *refs):
    given, outs, levels, sems = refs[: square - 1], refs[square - 1 : -2], refs[-2], refs[-1]
    me = lax.axis_index("dp")
    targets = [me] + [me ^ square ^ near for near in range(square)]
    copies = []
    for number, target in enumerate(targets):
        out = outs[number]
        copy = pltpu.make_async_copy(block_at(grads, target, out.shape[0]), out, sems.at[number])
        copy.start()
        copies.append(copy)
    lanes = lax.broadcasted_iota(jnp.int32, levels.shape, 1)
    peaks = jnp.zeros(levels.shape, jnp.float32)
    for near in range(1, square):
        peaks = jnp.where(lanes == (me ^ near), largest(given[near - 1]), peaks)
    for number, target in enumerate(targets):
        copies[number].wait()
        peaks = jnp.where(lanes == target, largest(outs[number]), peaks)
    counts = [jnp.zeros(levels.shape, jnp.int32) for _ in range(4)]
    for power in range(low_power, high_power):
        counts[power % 4] += (peaks >= jnp.float32(2.0**power)).astype(jnp.int32)
    levels[...] = (counts[0] + counts[1]) + (counts[2] + counts[3])


def pack(grads, rows, given):
    width = grads.shape[-1]
    vmem = pl.BlockSpec(memory_space=pltpu.VMEM)
    block = jax.ShapeDtypeStruct((rows, width), grads.dtype)
    count = square + 1 if given else square - 1
    levels = [jax.ShapeDtypeStruct((8, rows), jnp.int32)] if given else []
    return pl.pallas_call(
        second_kernel if given else first_kernel,
        out_shape=[block] * count + levels,
        in_specs=[pl.BlockSpec(memory_space=pltpu.HBM)] + [vmem] * len(given),
        out_specs=[vmem] * (count + len(levels)),
        scratch_shapes=[pltpu.SemaphoreType.DMA((count,))],
        compiler_params=pltpu.CompilerParams(vmem_limit_bytes=8 * 2**20),
        name="pack_rest" if given else "pack_own",
    )(pltpu.with_memory_space_constraint(grads, pltpu.HBM), *given)


def noise_of(codes, columns):
    mixed = codes + columns
    mixed = jnp.bitwise_xor(mixed, jnp.right_shift(mixed, 13))
    mixed = mixed * 1103515245
    mixed = jnp.bitwise_xor(mixed, jnp.right_shift(mixed, 16))
    return jnp.bitwise_and(jnp.right_shift(mixed, 12), 255).astype(jnp.float32) * (1.0 / 256.0)


def fill_codes(far, notes, codes):
    seeds = jnp.concatenate([note[far : far + 1, :] for note in notes] * 2)
    codes[...] = jnp.transpose(seeds) * 747796405 + 1013904223


def noise_kernel(far, *refs):
    notes, out, codes = refs[:square], refs[square], refs[square + 1]
    fill_codes(far, notes, codes)
    height, width = 16, out.shape[2]
    columns = lax.broadcasted_iota(jnp.int32, (1, width), 1) * 747796405

    def step(index, carry):
        span = pl.ds(pl.multiple_of(index * height, height), height)
        for near in range(square):
            out[near, span, :] = noise_of(codes[span, near : near + 1], columns).astype(jnp.bfloat16)
        return carry

    lax.fori_loop(0, out.shape[1] // height, step, 0)


def make_noise(far, notes, rows, width):
    vmem = pl.BlockSpec(memory_space=pltpu.VMEM)
    return pl.pallas_call(
        functools.partial(noise_kernel, far),
        out_shape=jax.ShapeDtypeStruct((square, rows, width), jnp.bfloat16),
        in_specs=[vmem] * square,
        out_specs=vmem,
        scratch_shapes=[pltpu.VMEM((rows, 2 * square), jnp.int32)],
        compiler_params=pltpu.CompilerParams(vmem_limit_bytes=8 * 2**20),
        name="noise",
    )(*notes)


def sum_kernel(far, rows, *refs):
    notes, raws, rest = refs[:square], refs[square : 2 * square], refs[2 * square :]
    noise, out, codes = (None, *rest) if far == 0 else (*rest, None)
    target = lax.axis_index("dp") ^ (far * square)
    counts = notes[0][2:3, :]
    for note in notes[1:]:
        counts = jnp.maximum(counts, note[2:3, :])
    lanes = lax.broadcasted_iota(jnp.int32, counts.shape, 1)
    reached = jnp.where(lanes == target, counts, 0).astype(jnp.float32)
    exponent = jnp.max(reached, axis=1, keepdims=True).astype(jnp.int32) + (low_power - level_bits)
    inverse_step = power_of_two(-exponent)
    height, width = 16, raws[0].shape[1]
    columns = lax.broadcasted_iota(jnp.int32, (1, width), 1) * 747796405
    if noise is None:
        fill_codes(far, notes, codes)

    def step(index, carry):
        span = pl.ds(pl.multiple_of(index * height, height), height)
        total = jnp.zeros((height, width), jnp.float32)
        for near in range(square):
            if noise is None:
                drawn = noise_of(codes[span, near : near + 1], columns)
            else:
                drawn = noise[near, span, :].astype(jnp.float32)
            scaled = raws[near][span, :].astype(jnp.float32) * inverse_step
            floor_part = jnp.floor(scaled)
            total = total + (floor_part + jnp.floor(scaled - floor_part + drawn))
        out[span, :] = total.astype(jnp.bfloat16)
        return carry

    lax.fori_loop(0, rows // height, step, 0)
    if out.shape[0] > rows:
        tail = (out.shape[0] - rows, width)
        out[rows:, :] = jnp.broadcast_to(power_of_two(exponent), tail).astype(jnp.bfloat16)


def sum_counts(far, notes, raws, noise, extra):
    rows, width = raws[0].shape
    vmem = pl.BlockSpec(memory_space=pltpu.VMEM)
    more = [noise] if far else []
    return pl.pallas_call(
        functools.partial(sum_kernel, far, rows),
        out_shape=jax.ShapeDtypeStruct((rows + extra, width), jnp.bfloat16),
        in_specs=[vmem] * (2 * square + len(more)),
        out_specs=vmem,
        scratch_shapes=[] if far else [pltpu.VMEM((rows, 2 * square), jnp.int32)],
        compiler_params=pltpu.CompilerParams(vmem_limit_bytes=8 * 2**20),
        name="sum_far" if far else "sum_near",
    )(*notes, *raws, *more)


def update_kernel(dp_count, slots, own, beside, across, arrived, weight, *refs):
    mean, updated, step, means, news, size_out, sems, size_sem = refs
    place = lax.axis_index("expert")
    positions = lax.broadcasted_iota(jnp.int32, slots.shape, 1)
    turns = jnp.where(slots[...] == place, positions ^ place, 0).astype(jnp.float32)
    turn = jnp.max(turns, axis=1, keepdims=True)
    rows = arrived.shape[0]

    def nearby(span):
        held, swapped, crossed = (ref[span, :].astype(jnp.float32) for ref in (own, beside, across))
        return jnp.where(turn == 0, held, jnp.where(turn == 1, swapped, crossed))

    size = nearby(slice(rows, own.shape[0]))[0:1, :]
    size_out[...] = size[:, 0:1]
    size_copy = pltpu.make_async_copy(size_out, step, size_sem)
    size_copy.start()
    scale = size * (1.0 / dp_count)
    parts = sems.shape[1]
    height = rows // parts
    copies = [size_copy]
    for part in range(parts):
        span = slice(part * height, (part + 1) * height)
        averaged = (nearby(span) + arrived[span, :].astype(jnp.float32)) * scale
        means[span, :] = averaged
        news[span, :] = weight[0, span, :] - learn_rate * averaged
        for number, (source, target) in enumerate(((means, mean), (news, updated))):
            copy = pltpu.make_async_copy(
                source.at[pl.ds(part * height, height), :],
                target.at[0, pl.ds(part * height, height), :],
                sems.at[number, part],
            )
            copy.start()
            copies.append(copy)
    for copy in copies:
        copy.wait()


def update(slots, own, beside, across, arrived, weight, dp_count):
    rows, width = arrived.shape
    parts = 4
    vmem = pl.BlockSpec(memory_space=pltpu.VMEM)
    hbm = pl.BlockSpec(memory_space=pltpu.HBM)
    block = jax.ShapeDtypeStruct((1, rows, width), jnp.float32)
    return pl.pallas_call(
        functools.partial(update_kernel, dp_count),
        out_shape=(block, block, jax.ShapeDtypeStruct((1, 1), jnp.float32)),
        in_specs=[vmem] * 6,
        out_specs=(hbm, hbm, hbm),
        scratch_shapes=[
            pltpu.VMEM((rows, width), jnp.float32),
            pltpu.VMEM((rows, width), jnp.float32),
            pltpu.VMEM((1, 1), jnp.float32),
            pltpu.SemaphoreType.DMA((2, parts)),
            pltpu.SemaphoreType.DMA,
        ],
        compiler_params=pltpu.CompilerParams(vmem_limit_bytes=8 * 2**20),
        name="update",
    )(slots[None], own, beside, across, arrived, weight)


def staged_body(expert_grads, round_offsets, slot_expert, master_weight):
    dp_count = lax.axis_size("dp")
    expert_count = lax.axis_size("expert")
    row_count, hidden = expert_grads.shape[2:]
    block_rows = row_count // dp_count
    me = lax.axis_index("dp")
    place = lax.axis_index("expert")
    offsets = round_offsets[0, 0].reshape(dp_count, block_rows)

    def pick(array, index):
        return lax.dynamic_index_in_dim(array, index, 0, keepdims=False)

    after = jnp.arange(expert_count)[None, :] > jnp.arange(expert_count)[:, None]
    weights = jnp.array([6, 2, 1, 0], jnp.int32)[:, None]
    lower = (slot_expert[:, None] > slot_expert[None, :]) & after
    branch = jnp.sum(jnp.where(lower, weights, 0))
    near_blocks = pack(expert_grads, block_rows, [])
    *rest, levels = pack(expert_grads, block_rows, near_blocks)
    twin = lax.ppermute(levels, "dp", flips(dp_count, square))
    levels = jnp.maximum(levels[0], twin[0])

    raw, notes = [[rest[0], *near_blocks], rest[1:]], []
    for near in range(square):
        seeds = [pick(offsets, (me ^ near) ^ (far * square)) for far in range(2)]
        note = jnp.concatenate([jnp.stack(seeds + [levels]), jnp.zeros((5, block_rows), jnp.int32)])
        if near:
            pairs = flips(dp_count, near)
            note = lax.ppermute(note, "dp", pairs)
            for far in range(2):
                raw[far][near] = lax.ppermute(raw[far][near], "dp", pairs)
        notes.append(note)

    wanted = slot_expert == (place ^ 2)
    crossing = jnp.sum(jnp.where(wanted, jnp.arange(expert_count), 0)) == place
    own = sum_counts(0, notes, raw[0], None, 8)
    beside = lax.ppermute(own, "expert", flips(expert_count, 1))
    across_wants = jnp.where(crossing, own, beside)
    across = lax.ppermute(across_wants, "expert", flips(expert_count, 2))
    noise = make_noise(1, notes, block_rows, hidden)
    message = sum_counts(1, notes, raw[1], noise, 0)

    def route(order):
        pairs = [
            (block * expert_count + slot, (block ^ square) * expert_count + order[slot])
            for block in range(dp_count)
            for slot in range(expert_count)
        ]
        return lambda parts: lax.ppermute(parts, ("dp", "expert"), pairs)

    orders = itertools.permutations(range(expert_count))
    arrived = lax.switch(branch, [route(order) for order in orders], message)
    return update(slot_expert, own, beside, across, arrived, master_weight, dp_count)


def solution(mesh):
    staged = mesh.shape["dp"] == 2 * square and mesh.shape["expert"] == 4
    return jax.shard_map(
        staged_body if staged else general_body,
        mesh=mesh,
        in_specs=(
            P("dp", "expert", None, None),
            P("dp", "expert", None),
            P(),
            P("expert", "dp", None),
        ),
        out_specs=(P("expert", "dp", None), P("expert", "dp", None), P("expert", "dp")),
        check_vma=False,
    )
```

```python
import functools
import itertools

import jax
import jax.numpy as jnp
from jax import lax
from jax.experimental import pallas as pl
from jax.experimental.pallas import tpu as pltpu
from jax.sharding import PartitionSpec as P

level_bits = 6
low_power = -30
high_power = 30
learn_rate = 0.05
field_base = 32768
count_shift = 64
square = 4


def power_steps(maxima):
    powers = jnp.array([2.0**exponent for exponent in range(low_power, high_power)], jnp.float32)
    reached = maxima[..., None] >= powers
    doubled = jnp.prod(jnp.where(reached, jnp.float32(2.0), jnp.float32(1.0)), axis=-1)
    return 2.0 ** (low_power - level_bits) * doubled


def dither(element_code):
    mixed = element_code * 747796405 + 1013904223
    mixed = jnp.bitwise_xor(mixed, jnp.right_shift(mixed, 13))
    mixed = mixed * 1103515245
    mixed = jnp.bitwise_xor(mixed, jnp.right_shift(mixed, 16))
    return jnp.bitwise_and(jnp.right_shift(mixed, 12), 255).astype(jnp.float32) / 256.0


def quantize(values, inverse_step, offsets):
    columns = lax.broadcasted_iota(jnp.int32, (1, values.shape[-1]), 1)
    element_code = offsets[..., None] + columns
    scaled = values.astype(jnp.float32) * inverse_step
    floor_part = jnp.floor(scaled)
    return floor_part + jnp.floor(scaled - floor_part + dither(element_code))


def apply_update(mean_grad, master_weight):
    return mean_grad, master_weight - learn_rate * mean_grad


def general_body(expert_grads, round_offsets, slot_expert, master_weight):
    dp_count = lax.axis_size("dp")
    local_grads = expert_grads[0]
    slot_count, row_count, hidden = local_grads.shape
    block_rows = row_count // dp_count
    shaped = local_grads.reshape(slot_count, dp_count, block_rows, hidden)
    maxima = lax.pmax(jnp.max(jnp.abs(shaped), axis=(2, 3)).astype(jnp.float32), "dp")
    all_steps = power_steps(maxima)
    counts = quantize(
        shaped,
        (1.0 / all_steps)[:, :, None, None],
        round_offsets[0].reshape(slot_count, dp_count, block_rows),
    ).astype(jnp.int32).reshape(slot_count, row_count, hidden)
    half = hidden // 2
    words = (counts[:, :, :half] + count_shift) * field_base + (counts[:, :, half:] + count_shift)
    summed = lax.psum_scatter(words, "dp", scatter_dimension=1, tiled=True)
    upper = jnp.right_shift(summed, 15) - count_shift * dp_count
    lower = jnp.bitwise_and(summed, field_base - 1) - count_shift * dp_count
    totals = jnp.concatenate([upper, lower], axis=2)
    step_sizes = lax.dynamic_slice_in_dim(all_steps, lax.axis_index("dp"), 1, 1)
    mean_slot = totals.astype(jnp.float32) * (step_sizes / dp_count)[..., None]
    gathered = lax.all_gather(mean_slot, "expert", axis=0, tiled=True)
    gathered_steps = lax.all_gather(step_sizes, "expert", axis=0, tiled=True)
    wanted = lax.axis_index("expert") * slot_count + lax.broadcasted_iota(
        jnp.int32, (slot_count, 1), 0
    )
    positions = lax.broadcasted_iota(jnp.int32, (1, slot_expert.shape[0]), 1)
    holder = jnp.sum(jnp.where(slot_expert[None, :] == wanted, positions, 0), axis=1)
    mean_grad, new_weight = apply_update(gathered[holder], master_weight)
    return mean_grad, new_weight, gathered_steps[holder]


def flips(count, mask):
    return [(index, index ^ mask) for index in range(count)]


def power_of_two(exponent):
    result = jnp.ones(exponent.shape, jnp.float32)
    size = jnp.abs(exponent)
    for bit in range(6):
        factor = jnp.where(exponent < 0, jnp.float32(2.0 ** -(2**bit)), jnp.float32(2.0 ** (2**bit)))
        result = result * jnp.where((size >> bit) & 1 == 1, factor, jnp.float32(1.0))
    return result


def block_at(grads, target, rows):
    return grads.at[0, 0, pl.ds(pl.multiple_of(target * rows, rows), rows), :]


def largest(ref):
    height = 16
    best = jnp.abs(ref[0:height, :])
    for row in range(height, ref.shape[0], height):
        best = jnp.maximum(best, jnp.abs(ref[row : row + height, :]))
    best = jnp.max(best.astype(jnp.float32), axis=0, keepdims=True)
    return jnp.max(best, axis=1, keepdims=True)


def first_kernel(grads, *refs):
    outs, sems = refs[:-1], refs[-1]
    me = lax.axis_index("dp")
    copies = []
    for number, out in enumerate(outs):
        source = block_at(grads, me ^ (number + 1), out.shape[0])
        copies.append(pltpu.make_async_copy(source, out, sems.at[number]))
        copies[-1].start()
    for copy in copies:
        copy.wait()


def second_kernel(given_count, grads, offsets, *refs):
    given, outs, rest = refs[:given_count], refs[given_count:-3], refs[-3:]
    mine, posted, sems = rest
    me = lax.axis_index("dp")
    targets = [me ^ turn for turn in (0, *range(given_count + 1, 2 * square))]
    copies = []
    for number, target in enumerate(targets):
        source = block_at(grads, target, outs[number].shape[0])
        copies.append(pltpu.make_async_copy(source, outs[number], sems.at[number]))
        copies[-1].start()
    for row, turn in enumerate((0, square, 2, 2 ^ square)):
        mine[row : row + 1, :] = offsets[pl.ds(me ^ turn, 1), :]
        posted[row : row + 1, :] = offsets[pl.ds(me ^ 1 ^ turn, 1), :]
    shape = (mine.shape[0] - square, mine.shape[1])
    lanes = lax.broadcasted_iota(jnp.int32, shape, 1)
    peaks = jnp.zeros(shape, jnp.float32)
    for number in range(given_count):
        peaks = jnp.where(lanes == (me ^ (number + 1)), largest(given[number]), peaks)
    for number, target in enumerate(targets):
        copies[number].wait()
        peaks = jnp.where(lanes == target, largest(outs[number]), peaks)
    counts = [jnp.zeros(shape, jnp.int32) for _ in range(4)]
    for power in range(low_power, high_power):
        counts[power % 4] += (peaks >= jnp.float32(2.0**power)).astype(jnp.int32)
    levels = (counts[0] + counts[1]) + (counts[2] + counts[3])
    mine[square:, :] = levels
    posted[square:, :] = levels


def pack_first(grads, rows, count):
    vmem = pl.BlockSpec(memory_space=pltpu.VMEM)
    return pl.pallas_call(
        first_kernel,
        out_shape=[jax.ShapeDtypeStruct((rows, grads.shape[-1]), grads.dtype)] * count,
        in_specs=[pl.BlockSpec(memory_space=pltpu.HBM)],
        out_specs=[vmem] * count,
        scratch_shapes=[pltpu.SemaphoreType.DMA((count,))],
        compiler_params=pltpu.CompilerParams(vmem_limit_bytes=8 * 2**20),
        name="pack_first",
    )(pltpu.with_memory_space_constraint(grads, pltpu.HBM))


def pack_second(grads, offsets, given):
    rows, width = given[0].shape
    count = 2 * square - len(given)
    vmem = pl.BlockSpec(memory_space=pltpu.VMEM)
    block = jax.ShapeDtypeStruct((rows, width), grads.dtype)
    note = jax.ShapeDtypeStruct((8, rows), jnp.int32)
    return pl.pallas_call(
        functools.partial(second_kernel, len(given)),
        out_shape=[block] * count + [note] * 2,
        in_specs=[pl.BlockSpec(memory_space=pltpu.HBM)] + [vmem] * (1 + len(given)),
        out_specs=[vmem] * (count + 2),
        scratch_shapes=[pltpu.SemaphoreType.DMA((count,))],
        compiler_params=pltpu.CompilerParams(vmem_limit_bytes=8 * 2**20),
        name="pack_second",
    )(pltpu.with_memory_space_constraint(grads, pltpu.HBM), offsets, *given)


def noise_of(codes, columns):
    mixed = codes + columns
    mixed = jnp.bitwise_xor(mixed, jnp.right_shift(mixed, 13))
    mixed = mixed * 1103515245
    mixed = jnp.bitwise_xor(mixed, jnp.right_shift(mixed, 16))
    return jnp.bitwise_and(jnp.right_shift(mixed, 12), 255).astype(jnp.float32) * (1.0 / 256.0)


def noise_kernel(far, mine, beside, above, out, codes):
    rows = [mine[far : far + 1, :], beside[far : far + 1, :]]
    rows += [above[far : far + 1, :], above[far + 2 : far + 3, :]]
    codes[...] = jnp.transpose(jnp.concatenate(rows * 2)) * 747796405 + 1013904223
    height, width = 16, out.shape[2]
    columns = lax.broadcasted_iota(jnp.int32, (1, width), 1) * 747796405

    def step(index, carry):
        span = pl.ds(pl.multiple_of(index * height, height), height)
        for near in range(square):
            out[near, span, :] = noise_of(codes[span, near : near + 1], columns).astype(jnp.bfloat16)
        return carry

    lax.fori_loop(0, out.shape[1] // height, step, 0)


def make_noise(far, notes, rows, width):
    vmem = pl.BlockSpec(memory_space=pltpu.VMEM)
    return pl.pallas_call(
        functools.partial(noise_kernel, far),
        out_shape=jax.ShapeDtypeStruct((square, rows, width), jnp.bfloat16),
        in_specs=[vmem] * len(notes),
        out_specs=vmem,
        scratch_shapes=[pltpu.VMEM((rows, 2 * square), jnp.int32)],
        compiler_params=pltpu.CompilerParams(vmem_limit_bytes=8 * 2**20),
        name="noise_far" if far else "noise_near",
    )(*notes)


def sum_kernel(far, levels, twin, noise, *refs):
    raws, out = refs[:square], refs[square]
    target = lax.axis_index("dp") ^ (far * square)
    counts = jnp.maximum(levels[0:1, :], twin[0:1, :])
    lanes = lax.broadcasted_iota(jnp.int32, counts.shape, 1)
    reached = jnp.where(lanes == target, counts, 0).astype(jnp.float32)
    exponent = jnp.max(reached, axis=1, keepdims=True).astype(jnp.int32) + (low_power - level_bits)
    inverse_step = power_of_two(-exponent)
    height = 16
    rows, width = raws[0].shape

    def step(index, carry):
        span = pl.ds(pl.multiple_of(index * height, height), height)
        total = jnp.zeros((height, width), jnp.float32)
        for near in range(square):
            drawn = noise[near, span, :].astype(jnp.float32)
            scaled = raws[near][span, :].astype(jnp.float32) * inverse_step
            floor_part = jnp.floor(scaled)
            total = total + (floor_part + jnp.floor(scaled - floor_part + drawn))
        out[span, :] = total.astype(jnp.bfloat16)
        return carry

    lax.fori_loop(0, rows // height, step, 0)
    if out.shape[0] > rows:
        tail = (out.shape[0] - rows, width)
        out[rows:, :] = jnp.broadcast_to(power_of_two(exponent), tail).astype(jnp.bfloat16)


def sum_counts(far, levels, twin, noise, raws, extra):
    rows, width = raws[0].shape
    vmem = pl.BlockSpec(memory_space=pltpu.VMEM)
    return pl.pallas_call(
        functools.partial(sum_kernel, far),
        out_shape=jax.ShapeDtypeStruct((rows + extra, width), jnp.bfloat16),
        in_specs=[vmem] * (3 + square),
        out_specs=vmem,
        compiler_params=pltpu.CompilerParams(vmem_limit_bytes=8 * 2**20),
        name="sum_far" if far else "sum_near",
    )(levels, twin, noise, *raws)


def update_kernel(dp_count, slots, own, beside, across, arrived, weight, *refs):
    mean, updated, step, means, news, size_out, sems, size_sem = refs
    place = lax.axis_index("expert")
    positions = lax.broadcasted_iota(jnp.int32, slots.shape, 1)
    turns = jnp.where(slots[...] == place, positions ^ place, 0).astype(jnp.float32)
    turn = jnp.max(turns, axis=1, keepdims=True)
    rows = arrived.shape[0]

    def nearby(span):
        held, swapped, crossed = (ref[span, :].astype(jnp.float32) for ref in (own, beside, across))
        return jnp.where(turn == 0, held, jnp.where(turn == 1, swapped, crossed))

    size = nearby(slice(rows, own.shape[0]))[0:1, :]
    size_out[...] = size[:, 0:1]
    size_copy = pltpu.make_async_copy(size_out, step, size_sem)
    size_copy.start()
    scale = size * (1.0 / dp_count)
    parts = sems.shape[1]
    height = rows // parts
    copies = [size_copy]
    for part in range(parts):
        span = slice(part * height, (part + 1) * height)
        averaged = (nearby(span) + arrived[span, :].astype(jnp.float32)) * scale
        means[span, :] = averaged
        news[span, :] = weight[0, span, :] - learn_rate * averaged
        for number, (source, target) in enumerate(((means, mean), (news, updated))):
            copy = pltpu.make_async_copy(
                source.at[pl.ds(part * height, height), :],
                target.at[0, pl.ds(part * height, height), :],
                sems.at[number, part],
            )
            copy.start()
            copies.append(copy)
    for copy in copies:
        copy.wait()


def update(slots, own, beside, across, arrived, weight, dp_count):
    rows, width = arrived.shape
    parts = 8
    vmem = pl.BlockSpec(memory_space=pltpu.VMEM)
    hbm = pl.BlockSpec(memory_space=pltpu.HBM)
    block = jax.ShapeDtypeStruct((1, rows, width), jnp.float32)
    return pl.pallas_call(
        functools.partial(update_kernel, dp_count),
        out_shape=(block, block, jax.ShapeDtypeStruct((1, 1), jnp.float32)),
        in_specs=[vmem] * 6,
        out_specs=(hbm, hbm, hbm),
        scratch_shapes=[
            pltpu.VMEM((rows, width), jnp.float32),
            pltpu.VMEM((rows, width), jnp.float32),
            pltpu.VMEM((1, 1), jnp.float32),
            pltpu.SemaphoreType.DMA((2, parts)),
            pltpu.SemaphoreType.DMA,
        ],
        compiler_params=pltpu.CompilerParams(vmem_limit_bytes=8 * 2**20),
        name="update",
    )(slots[None], own, beside, across, arrived, weight)


def staged_body(expert_grads, round_offsets, slot_expert, master_weight):
    dp_count = lax.axis_size("dp")
    expert_count = lax.axis_size("expert")
    row_count, hidden = expert_grads.shape[2:]
    block_rows = row_count // dp_count
    place = lax.axis_index("expert")
    offsets = round_offsets[0, 0].reshape(dp_count, block_rows)

    after = jnp.arange(expert_count)[None, :] > jnp.arange(expert_count)[:, None]
    weights = jnp.array([6, 2, 1, 0], jnp.int32)[:, None]
    lower = (slot_expert[:, None] > slot_expert[None, :]) & after
    branch = jnp.sum(jnp.where(lower, weights, 0))
    near_blocks = pack_first(expert_grads, block_rows, 2)
    here, diagonal, *far_blocks, mine, posted = pack_second(expert_grads, offsets, near_blocks)
    raw = [[here, near_blocks[0], near_blocks[1], diagonal], far_blocks]
    for far in range(2):
        for near in range(1, square):
            raw[far][near] = lax.ppermute(raw[far][near], "dp", flips(dp_count, near))

    aside = lax.ppermute(posted, "dp", flips(dp_count, 1))
    levels = jnp.maximum(mine[square:], aside[square:])
    upward = jnp.concatenate([mine[2:square], aside[2:square], levels])
    above = lax.ppermute(upward, "dp", flips(dp_count, 2))
    levels = jnp.maximum(levels, above[square:])
    twin = lax.ppermute(levels, "dp", flips(dp_count, square))
    noise = []
    for far in range(2):
        noise.append(make_noise(far, (mine, aside, above), block_rows, hidden))

    wanted = slot_expert == (place ^ 2)
    crossing = jnp.sum(jnp.where(wanted, jnp.arange(expert_count), 0)) == place
    own = sum_counts(0, levels, twin, noise[0], raw[0], 8)
    beside = lax.ppermute(own, "expert", flips(expert_count, 1))
    across_wants = jnp.where(crossing, own, beside)
    across = lax.ppermute(across_wants, "expert", flips(expert_count, 2))
    message = sum_counts(1, levels, twin, noise[1], raw[1], 0)

    def route(order):
        pairs = [
            (block * expert_count + slot, (block ^ square) * expert_count + order[slot])
            for block in range(dp_count)
            for slot in range(expert_count)
        ]
        return lambda parts: lax.ppermute(parts, ("dp", "expert"), pairs)

    orders = itertools.permutations(range(expert_count))
    arrived = lax.switch(branch, [route(order) for order in orders], message)
    return update(slot_expert, own, beside, across, arrived, master_weight, dp_count)


def solution(mesh):
    staged = mesh.shape["dp"] == 2 * square and mesh.shape["expert"] == 4
    return jax.shard_map(
        staged_body if staged else general_body,
        mesh=mesh,
        in_specs=(
            P("dp", "expert", None, None),
            P("dp", "expert", None),
            P(),
            P("expert", "dp", None),
        ),
        out_specs=(P("expert", "dp", None), P("expert", "dp", None), P("expert", "dp")),
        check_vma=False,
    )
```

```python
import functools
import itertools

import jax
import jax.numpy as jnp
from jax import lax
from jax.experimental import pallas as pl
from jax.experimental.pallas import tpu as pltpu
from jax.sharding import PartitionSpec as P

level_bits = 6
low_power = -30
high_power = 30
learn_rate = 0.05
field_base = 32768
count_shift = 64
square = 4


def power_steps(maxima):
    powers = jnp.array([2.0**exponent for exponent in range(low_power, high_power)], jnp.float32)
    reached = maxima[..., None] >= powers
    doubled = jnp.prod(jnp.where(reached, jnp.float32(2.0), jnp.float32(1.0)), axis=-1)
    return 2.0 ** (low_power - level_bits) * doubled


def dither(element_code):
    mixed = element_code * 747796405 + 1013904223
    mixed = jnp.bitwise_xor(mixed, jnp.right_shift(mixed, 13))
    mixed = mixed * 1103515245
    mixed = jnp.bitwise_xor(mixed, jnp.right_shift(mixed, 16))
    return jnp.bitwise_and(jnp.right_shift(mixed, 12), 255).astype(jnp.float32) / 256.0


def quantize(values, inverse_step, offsets):
    columns = lax.broadcasted_iota(jnp.int32, (1, values.shape[-1]), 1)
    element_code = offsets[..., None] + columns
    scaled = values.astype(jnp.float32) * inverse_step
    floor_part = jnp.floor(scaled)
    return floor_part + jnp.floor(scaled - floor_part + dither(element_code))


def apply_update(mean_grad, master_weight):
    return mean_grad, master_weight - learn_rate * mean_grad


def general_body(expert_grads, round_offsets, slot_expert, master_weight):
    dp_count = lax.axis_size("dp")
    local_grads = expert_grads[0]
    slot_count, row_count, hidden = local_grads.shape
    block_rows = row_count // dp_count
    shaped = local_grads.reshape(slot_count, dp_count, block_rows, hidden)
    maxima = lax.pmax(jnp.max(jnp.abs(shaped), axis=(2, 3)).astype(jnp.float32), "dp")
    all_steps = power_steps(maxima)
    counts = quantize(
        shaped,
        (1.0 / all_steps)[:, :, None, None],
        round_offsets[0].reshape(slot_count, dp_count, block_rows),
    ).astype(jnp.int32).reshape(slot_count, row_count, hidden)
    half = hidden // 2
    words = (counts[:, :, :half] + count_shift) * field_base + (counts[:, :, half:] + count_shift)
    summed = lax.psum_scatter(words, "dp", scatter_dimension=1, tiled=True)
    upper = jnp.right_shift(summed, 15) - count_shift * dp_count
    lower = jnp.bitwise_and(summed, field_base - 1) - count_shift * dp_count
    totals = jnp.concatenate([upper, lower], axis=2)
    step_sizes = lax.dynamic_slice_in_dim(all_steps, lax.axis_index("dp"), 1, 1)
    mean_slot = totals.astype(jnp.float32) * (step_sizes / dp_count)[..., None]
    gathered = lax.all_gather(mean_slot, "expert", axis=0, tiled=True)
    gathered_steps = lax.all_gather(step_sizes, "expert", axis=0, tiled=True)
    wanted = lax.axis_index("expert") * slot_count + lax.broadcasted_iota(
        jnp.int32, (slot_count, 1), 0
    )
    positions = lax.broadcasted_iota(jnp.int32, (1, slot_expert.shape[0]), 1)
    holder = jnp.sum(jnp.where(slot_expert[None, :] == wanted, positions, 0), axis=1)
    mean_grad, new_weight = apply_update(gathered[holder], master_weight)
    return mean_grad, new_weight, gathered_steps[holder]


def flips(count, mask):
    return [(index, index ^ mask) for index in range(count)]


def power_of_two(exponent):
    result = jnp.ones(exponent.shape, jnp.float32)
    size = jnp.abs(exponent)
    for bit in range(6):
        factor = jnp.where(exponent < 0, jnp.float32(2.0 ** -(2**bit)), jnp.float32(2.0 ** (2**bit)))
        result = result * jnp.where((size >> bit) & 1 == 1, factor, jnp.float32(1.0))
    return result


def block_at(grads, target, rows):
    return grads.at[0, 0, pl.ds(pl.multiple_of(target * rows, rows), rows), :]


def largest(ref):
    height = 16
    best = jnp.abs(ref[0:height, :])
    for row in range(height, ref.shape[0], height):
        best = jnp.maximum(best, jnp.abs(ref[row : row + height, :]))
    best = jnp.max(best.astype(jnp.float32), axis=0, keepdims=True)
    return jnp.max(best, axis=1, keepdims=True)


def first_kernel(grads, *refs):
    outs, sems = refs[:-1], refs[-1]
    me = lax.axis_index("dp")
    copies = []
    for number, out in enumerate(outs):
        source = block_at(grads, me ^ (number + 1), out.shape[0])
        copies.append(pltpu.make_async_copy(source, out, sems.at[number]))
        copies[-1].start()
    for copy in copies:
        copy.wait()


def is_inner(index):
    return ((index >> 1) ^ (index >> 2)) & 1


def second_kernel(given_count, grads, offsets, *refs):
    given, outs, (posted, sems) = refs[:given_count], refs[given_count:-2], refs[-2:]
    me = lax.axis_index("dp")
    inner = is_inner(me)
    targets = [me ^ turn for turn in (0, 3, 4, 5)] + [me ^ (7 - inner), me ^ (6 + inner)]
    copies = []
    for number, target in enumerate(targets):
        source = block_at(grads, target, outs[number].shape[0])
        copies.append(pltpu.make_async_copy(source, outs[number], sems.at[number]))
        copies[-1].start()
    count = offsets.shape[0]
    posted[0:count, :] = offsets[...]
    lanes = lax.broadcasted_iota(jnp.int32, offsets.shape, 1)
    peaks = jnp.zeros(offsets.shape, jnp.float32)
    for number in range(given_count):
        peaks = jnp.where(lanes == (me ^ (number + 1)), largest(given[number]), peaks)
    for number, target in enumerate(targets):
        copies[number].wait()
        peaks = jnp.where(lanes == target, largest(outs[number]), peaks)
    counts = [jnp.zeros(offsets.shape, jnp.int32) for _ in range(4)]
    for power in range(low_power, high_power):
        counts[power % 4] += (peaks >= jnp.float32(2.0**power)).astype(jnp.int32)
    posted[count:, :] = (counts[0] + counts[1]) + (counts[2] + counts[3])


def note_kernel(posted, twin, mine, aside):
    me = lax.axis_index("dp")
    count = posted.shape[0] // 2

    def fill(out, row, target):
        out[row : row + 1, :] = posted[pl.ds(target, 1), :]
        far = posted[pl.ds(target ^ 6, 1), :]
        out[row + 1 : row + 2, :] = jnp.where(is_inner(target) == 1, twin[pl.ds(target, 1), :], far)

    levels = jnp.maximum(posted[count : count + 4, :], twin[count : count + 4, :])
    for out, turn in ((mine, 0), (aside, 1)):
        fill(out, 0, me ^ turn)
        fill(out, 2, me ^ turn ^ 2)
        out[4:8, :] = levels


def make_notes(posted, twin):
    vmem = pl.BlockSpec(memory_space=pltpu.VMEM)
    note = jax.ShapeDtypeStruct((8, posted.shape[1]), jnp.int32)
    return pl.pallas_call(
        note_kernel,
        out_shape=[note] * 2,
        in_specs=[vmem] * 2,
        out_specs=[vmem] * 2,
        compiler_params=pltpu.CompilerParams(vmem_limit_bytes=8 * 2**20),
        name="notes",
    )(posted, twin)


def pack_first(grads, rows, count):
    vmem = pl.BlockSpec(memory_space=pltpu.VMEM)
    return pl.pallas_call(
        first_kernel,
        out_shape=[jax.ShapeDtypeStruct((rows, grads.shape[-1]), grads.dtype)] * count,
        in_specs=[pl.BlockSpec(memory_space=pltpu.HBM)],
        out_specs=[vmem] * count,
        scratch_shapes=[pltpu.SemaphoreType.DMA((count,))],
        compiler_params=pltpu.CompilerParams(vmem_limit_bytes=8 * 2**20),
        name="pack_first",
    )(pltpu.with_memory_space_constraint(grads, pltpu.HBM))


def pack_second(grads, offsets, given):
    rows, width = given[0].shape
    count = 2 * square - len(given)
    vmem = pl.BlockSpec(memory_space=pltpu.VMEM)
    block = jax.ShapeDtypeStruct((rows, width), grads.dtype)
    posted = jax.ShapeDtypeStruct((2 * offsets.shape[0], rows), jnp.int32)
    return pl.pallas_call(
        functools.partial(second_kernel, len(given)),
        out_shape=[block] * count + [posted],
        in_specs=[pl.BlockSpec(memory_space=pltpu.HBM)] + [vmem] * (1 + len(given)),
        out_specs=[vmem] * (count + 1),
        scratch_shapes=[pltpu.SemaphoreType.DMA((count,))],
        compiler_params=pltpu.CompilerParams(vmem_limit_bytes=8 * 2**20),
        name="pack_second",
    )(pltpu.with_memory_space_constraint(grads, pltpu.HBM), offsets, *given)


def noise_of(codes, columns):
    mixed = codes + columns
    mixed = jnp.bitwise_xor(mixed, jnp.right_shift(mixed, 13))
    mixed = mixed * 1103515245
    mixed = jnp.bitwise_xor(mixed, jnp.right_shift(mixed, 16))
    return jnp.bitwise_and(jnp.right_shift(mixed, 12), 255).astype(jnp.float32) * (1.0 / 256.0)


def fill_codes(far, mine, aside, above, codes):
    rows = [mine[far : far + 1, :], aside[far : far + 1, :]]
    rows += [above[far : far + 1, :], above[far + 2 : far + 3, :]]
    if far:
        inner = is_inner(lax.axis_index("dp")) == 1
        here, y, z, diagonal = rows
        rows = [jnp.where(inner, diagonal, here), jnp.where(inner, z, y)]
        rows += [jnp.where(inner, here, z), jnp.where(inner, y, diagonal)]
    codes[...] = jnp.transpose(jnp.concatenate(rows * 2)) * 747796405 + 1013904223


def noise_kernel(mine, aside, above, out, codes):
    fill_codes(1, mine, aside, above, codes)
    height, width = 16, out.shape[2]
    columns = lax.broadcasted_iota(jnp.int32, (1, width), 1) * 747796405

    def step(index, carry):
        span = pl.ds(pl.multiple_of(index * height, height), height)
        for near in range(square):
            out[near, span, :] = noise_of(codes[span, near : near + 1], columns).astype(jnp.bfloat16)
        return carry

    lax.fori_loop(0, out.shape[1] // height, step, 0)


def far_noise(notes, rows, width):
    vmem = pl.BlockSpec(memory_space=pltpu.VMEM)
    return pl.pallas_call(
        noise_kernel,
        out_shape=jax.ShapeDtypeStruct((square, rows, width), jnp.bfloat16),
        in_specs=[vmem] * len(notes),
        out_specs=vmem,
        scratch_shapes=[pltpu.VMEM((rows, 2 * square), jnp.int32)],
        compiler_params=pltpu.CompilerParams(vmem_limit_bytes=8 * 2**20),
        name="noise",
    )(*notes)


def sum_kernel(far, rows, mine, upward, aside, above, *refs):
    me = lax.axis_index("dp")
    inner = is_inner(me) == 1
    if far:
        noise, stays, *raws, out = refs
        target = jnp.where(inner, me, me ^ 6)
    else:
        *raws, out, codes = refs
        target = me
        fill_codes(0, mine, aside, above, codes)
    counts = jnp.maximum(upward[square : square + 1, :], above[square : square + 1, :])
    lanes = lax.broadcasted_iota(jnp.int32, counts.shape, 1)
    reached = jnp.where(lanes == target, counts, 0).astype(jnp.float32)
    exponent = jnp.max(reached, axis=1, keepdims=True).astype(jnp.int32) + (low_power - level_bits)
    inverse_step = power_of_two(-exponent)
    height, width = 16, raws[0].shape[1]
    columns = lax.broadcasted_iota(jnp.int32, (1, width), 1) * 747796405

    def step(index, carry):
        span = pl.ds(pl.multiple_of(index * height, height), height)
        total = jnp.zeros((height, width), jnp.float32)
        for near in range(square):
            if far:
                drawn = noise[near, span, :].astype(jnp.float32)
            else:
                drawn = noise_of(codes[span, near : near + 1], columns)
            values = raws[near][span, :].astype(jnp.float32)
            if far and near == 0:
                values = jnp.where(inner, values, stays[span, :].astype(jnp.float32))
            scaled = values * inverse_step
            floor_part = jnp.floor(scaled)
            total = total + (floor_part + jnp.floor(scaled - floor_part + drawn))
        out[span, :] = total.astype(jnp.bfloat16)
        return carry

    lax.fori_loop(0, rows // height, step, 0)
    if out.shape[0] > rows:
        tail = (out.shape[0] - rows, width)
        out[rows:, :] = jnp.broadcast_to(power_of_two(exponent), tail).astype(jnp.bfloat16)


def sum_counts(far, notes, raws, extra):
    rows, width = raws[-1].shape
    vmem = pl.BlockSpec(memory_space=pltpu.VMEM)
    return pl.pallas_call(
        functools.partial(sum_kernel, far, rows),
        out_shape=jax.ShapeDtypeStruct((rows + extra, width), jnp.bfloat16),
        in_specs=[vmem] * (len(notes) + len(raws)),
        out_specs=vmem,
        scratch_shapes=[] if far else [pltpu.VMEM((rows, 2 * square), jnp.int32)],
        compiler_params=pltpu.CompilerParams(vmem_limit_bytes=8 * 2**20),
        name="sum_far" if far else "sum_near",
    )(*notes, *raws)


def update_kernel(dp_count, slots, own, beside, across, arrived, weight, *refs):
    mean, updated, step, means, news, size_out, sems, size_sem = refs
    place = lax.axis_index("expert")
    positions = lax.broadcasted_iota(jnp.int32, slots.shape, 1)
    turns = jnp.where(slots[...] == place, positions ^ place, 0).astype(jnp.float32)
    turn = jnp.max(turns, axis=1, keepdims=True)
    rows = arrived.shape[0]

    def nearby(span):
        held, swapped, crossed = (ref[span, :].astype(jnp.float32) for ref in (own, beside, across))
        return jnp.where(turn == 0, held, jnp.where(turn == 1, swapped, crossed))

    size = nearby(slice(rows, own.shape[0]))[0:1, :]
    size_out[...] = size[:, 0:1]
    size_copy = pltpu.make_async_copy(size_out, step, size_sem)
    size_copy.start()
    scale = size * (1.0 / dp_count)
    parts = sems.shape[1]
    height = rows // parts
    copies = [size_copy]
    for part in range(parts):
        span = slice(part * height, (part + 1) * height)
        averaged = (nearby(span) + arrived[span, :].astype(jnp.float32)) * scale
        means[span, :] = averaged
        news[span, :] = weight[0, span, :] - learn_rate * averaged
        for number, (source, target) in enumerate(((means, mean), (news, updated))):
            copy = pltpu.make_async_copy(
                source.at[pl.ds(part * height, height), :],
                target.at[0, pl.ds(part * height, height), :],
                sems.at[number, part],
            )
            copy.start()
            copies.append(copy)
    for copy in copies:
        copy.wait()


def update(slots, own, beside, across, arrived, weight, dp_count):
    rows, width = arrived.shape
    parts = 4
    vmem = pl.BlockSpec(memory_space=pltpu.VMEM)
    hbm = pl.BlockSpec(memory_space=pltpu.HBM)
    block = jax.ShapeDtypeStruct((1, rows, width), jnp.float32)
    return pl.pallas_call(
        functools.partial(update_kernel, dp_count),
        out_shape=(block, block, jax.ShapeDtypeStruct((1, 1), jnp.float32)),
        in_specs=[vmem] * 6,
        out_specs=(hbm, hbm, hbm),
        scratch_shapes=[
            pltpu.VMEM((rows, width), jnp.float32),
            pltpu.VMEM((rows, width), jnp.float32),
            pltpu.VMEM((1, 1), jnp.float32),
            pltpu.SemaphoreType.DMA((2, parts)),
            pltpu.SemaphoreType.DMA,
        ],
        compiler_params=pltpu.CompilerParams(vmem_limit_bytes=8 * 2**20),
        name="update",
    )(slots[None], own, beside, across, arrived, weight)


def staged_body(expert_grads, round_offsets, slot_expert, master_weight):
    dp_count = lax.axis_size("dp")
    expert_count = lax.axis_size("expert")
    row_count, hidden = expert_grads.shape[2:]
    block_rows = row_count // dp_count
    place = lax.axis_index("expert")
    offsets = round_offsets[0, 0].reshape(dp_count, block_rows)

    after = jnp.arange(expert_count)[None, :] > jnp.arange(expert_count)[:, None]
    weights = jnp.array([6, 2, 1, 0], jnp.int32)[:, None]
    lower = (slot_expert[:, None] > slot_expert[None, :]) & after
    branch = jnp.sum(jnp.where(lower, weights, 0))
    near_blocks = pack_first(expert_grads, block_rows, 2)
    packed = pack_second(expert_grads, offsets, near_blocks)
    here, diagonal, four, five, fa, last, posted = packed
    raw = [here, near_blocks[0], near_blocks[1], diagonal]
    for near in range(1, square):
        raw[near] = lax.ppermute(raw[near], "dp", flips(dp_count, near))

    def mixed(inner_turn, outer_turn):
        turns = [inner_turn if is_inner(index) else outer_turn for index in range(dp_count)]
        return [(index, index ^ turn) for index, turn in enumerate(turns) if turn]

    fa = lax.ppermute(fa, "dp", mixed(6, 1))
    four = lax.ppermute(four, "dp", mixed(2, 4))
    five = lax.ppermute(five, "dp", mixed(3, 5))
    crossed = lax.ppermute(last, "dp", mixed(7, 0))

    twin = lax.ppermute(posted, "dp", flips(dp_count, square))
    mine, sideways = make_notes(posted, twin)
    aside = lax.ppermute(sideways, "dp", flips(dp_count, 1))
    levels = jnp.maximum(mine[square:], aside[square:])
    upward = jnp.concatenate([mine[2:square], aside[2:square], levels])
    above = lax.ppermute(upward, "dp", flips(dp_count, 2))
    noise = far_noise((mine, aside, above), block_rows, hidden)

    wanted = slot_expert == (place ^ 2)
    crossing = jnp.sum(jnp.where(wanted, jnp.arange(expert_count), 0)) == place
    own = sum_counts(0, (mine, upward, aside, above), raw, 8)
    beside = lax.ppermute(own, "expert", flips(expert_count, 1))
    across_wants = jnp.where(crossing, own, beside)
    across = lax.ppermute(across_wants, "expert", flips(expert_count, 2))
    raws = (noise, last, crossed, fa, four, five)
    message = sum_counts(1, (mine, upward, aside, above), raws, 0)

    def route(order):
        pairs = [
            (block * expert_count + slot, (block if is_inner(block) else block ^ 6) * expert_count + order[slot])
            for block in range(dp_count)
            for slot in range(expert_count)
        ]
        return lambda parts: lax.ppermute(parts, ("dp", "expert"), pairs)

    orders = itertools.permutations(range(expert_count))
    arrived = lax.switch(branch, [route(order) for order in orders], message)
    return update(slot_expert, own, beside, across, arrived, master_weight, dp_count)


def solution(mesh):
    staged = mesh.shape["dp"] == 2 * square and mesh.shape["expert"] == 4
    return jax.shard_map(
        staged_body if staged else general_body,
        mesh=mesh,
        in_specs=(
            P("dp", "expert", None, None),
            P("dp", "expert", None),
            P(),
            P("expert", "dp", None),
        ),
        out_specs=(P("expert", "dp", None), P("expert", "dp", None), P("expert", "dp")),
        check_vma=False,
    )
```

```python
import functools
import itertools

import jax
import jax.numpy as jnp
from jax import lax
from jax.experimental import pallas as pl
from jax.experimental.pallas import tpu as pltpu
from jax.sharding import PartitionSpec as P

level_bits = 6
low_power = -30
high_power = 30
learn_rate = 0.05
field_base = 32768
count_shift = 64
square = 4


def power_steps(maxima):
    powers = jnp.array([2.0**exponent for exponent in range(low_power, high_power)], jnp.float32)
    reached = maxima[..., None] >= powers
    doubled = jnp.prod(jnp.where(reached, jnp.float32(2.0), jnp.float32(1.0)), axis=-1)
    return 2.0 ** (low_power - level_bits) * doubled


def dither(element_code):
    mixed = element_code * 747796405 + 1013904223
    mixed = jnp.bitwise_xor(mixed, jnp.right_shift(mixed, 13))
    mixed = mixed * 1103515245
    mixed = jnp.bitwise_xor(mixed, jnp.right_shift(mixed, 16))
    return jnp.bitwise_and(jnp.right_shift(mixed, 12), 255).astype(jnp.float32) / 256.0


def quantize(values, inverse_step, offsets):
    columns = lax.broadcasted_iota(jnp.int32, (1, values.shape[-1]), 1)
    element_code = offsets[..., None] + columns
    scaled = values.astype(jnp.float32) * inverse_step
    floor_part = jnp.floor(scaled)
    return floor_part + jnp.floor(scaled - floor_part + dither(element_code))


def apply_update(mean_grad, master_weight):
    return mean_grad, master_weight - learn_rate * mean_grad


def general_body(expert_grads, round_offsets, slot_expert, master_weight):
    dp_count = lax.axis_size("dp")
    local_grads = expert_grads[0]
    slot_count, row_count, hidden = local_grads.shape
    block_rows = row_count // dp_count
    shaped = local_grads.reshape(slot_count, dp_count, block_rows, hidden)
    maxima = lax.pmax(jnp.max(jnp.abs(shaped), axis=(2, 3)).astype(jnp.float32), "dp")
    all_steps = power_steps(maxima)
    counts = quantize(
        shaped,
        (1.0 / all_steps)[:, :, None, None],
        round_offsets[0].reshape(slot_count, dp_count, block_rows),
    ).astype(jnp.int32).reshape(slot_count, row_count, hidden)
    half = hidden // 2
    words = (counts[:, :, :half] + count_shift) * field_base + (counts[:, :, half:] + count_shift)
    summed = lax.psum_scatter(words, "dp", scatter_dimension=1, tiled=True)
    upper = jnp.right_shift(summed, 15) - count_shift * dp_count
    lower = jnp.bitwise_and(summed, field_base - 1) - count_shift * dp_count
    totals = jnp.concatenate([upper, lower], axis=2)
    step_sizes = lax.dynamic_slice_in_dim(all_steps, lax.axis_index("dp"), 1, 1)
    mean_slot = totals.astype(jnp.float32) * (step_sizes / dp_count)[..., None]
    gathered = lax.all_gather(mean_slot, "expert", axis=0, tiled=True)
    gathered_steps = lax.all_gather(step_sizes, "expert", axis=0, tiled=True)
    wanted = lax.axis_index("expert") * slot_count + lax.broadcasted_iota(
        jnp.int32, (slot_count, 1), 0
    )
    positions = lax.broadcasted_iota(jnp.int32, (1, slot_expert.shape[0]), 1)
    holder = jnp.sum(jnp.where(slot_expert[None, :] == wanted, positions, 0), axis=1)
    mean_grad, new_weight = apply_update(gathered[holder], master_weight)
    return mean_grad, new_weight, gathered_steps[holder]


def flips(count, mask):
    return [(index, index ^ mask) for index in range(count)]


def power_of_two(exponent):
    result = jnp.ones(exponent.shape, jnp.float32)
    size = jnp.abs(exponent)
    for bit in range(6):
        factor = jnp.where(exponent < 0, jnp.float32(2.0 ** -(2**bit)), jnp.float32(2.0 ** (2**bit)))
        result = result * jnp.where((size >> bit) & 1 == 1, factor, jnp.float32(1.0))
    return result


def block_at(grads, target, rows):
    return grads.at[0, 0, pl.ds(pl.multiple_of(target * rows, rows), rows), :]


def largest(ref):
    height = 16
    best = jnp.abs(ref[0:height, :])
    for row in range(height, ref.shape[0], height):
        best = jnp.maximum(best, jnp.abs(ref[row : row + height, :]))
    best = jnp.max(best.astype(jnp.float32), axis=0, keepdims=True)
    return jnp.max(best, axis=1, keepdims=True)


def is_inner(index):
    return ((index >> 1) ^ (index >> 2)) & 1


def first_kernel(grads, *refs):
    outs, sems = refs[:-1], refs[-1]
    me = lax.axis_index("dp")
    copies = []
    targets = [me ^ 1, me ^ 2, me ^ (7 - is_inner(me))]
    for number, out in enumerate(outs):
        source = block_at(grads, targets[number], out.shape[0])
        copies.append(pltpu.make_async_copy(source, out, sems.at[number]))
        copies[-1].start()
    for copy in copies:
        copy.wait()


def second_kernel(given_count, grads, offsets, *refs):
    given, outs, (posted, sems) = refs[:given_count], refs[given_count:-2], refs[-2:]
    me = lax.axis_index("dp")
    inner = is_inner(me)
    targets = [me ^ turn for turn in (0, 3, 4, 5)] + [me ^ (6 + inner)]
    sources = [me ^ 1, me ^ 2, me ^ (7 - inner)]
    copies = []
    for number, target in enumerate(targets):
        source = block_at(grads, target, outs[number].shape[0])
        copies.append(pltpu.make_async_copy(source, outs[number], sems.at[number]))
        copies[-1].start()
    count = offsets.shape[0]
    posted[0:count, :] = offsets[...]
    lanes = lax.broadcasted_iota(jnp.int32, offsets.shape, 1)
    peaks = jnp.zeros(offsets.shape, jnp.float32)
    for number in range(given_count):
        peaks = jnp.where(lanes == sources[number], largest(given[number]), peaks)
    for number, target in enumerate(targets):
        copies[number].wait()
        peaks = jnp.where(lanes == target, largest(outs[number]), peaks)
    counts = [jnp.zeros(offsets.shape, jnp.int32) for _ in range(4)]
    for power in range(low_power, high_power):
        counts[power % 4] += (peaks >= jnp.float32(2.0**power)).astype(jnp.int32)
    posted[count:, :] = (counts[0] + counts[1]) + (counts[2] + counts[3])


def note_kernel(posted, twin, mine, aside):
    me = lax.axis_index("dp")
    count = posted.shape[0] // 2

    def fill(out, row, target):
        out[row : row + 1, :] = posted[pl.ds(target, 1), :]
        far = posted[pl.ds(target ^ 6, 1), :]
        out[row + 1 : row + 2, :] = jnp.where(is_inner(target) == 1, twin[pl.ds(target, 1), :], far)

    levels = jnp.maximum(posted[count : count + 4, :], twin[count : count + 4, :])
    for out, turn in ((mine, 0), (aside, 2)):
        fill(out, 0, me ^ turn)
        fill(out, 2, me ^ turn ^ 1)
        out[4:8, :] = levels


def make_notes(posted, twin):
    vmem = pl.BlockSpec(memory_space=pltpu.VMEM)
    note = jax.ShapeDtypeStruct((8, posted.shape[1]), jnp.int32)
    return pl.pallas_call(
        note_kernel,
        out_shape=[note] * 2,
        in_specs=[vmem] * 2,
        out_specs=[vmem] * 2,
        compiler_params=pltpu.CompilerParams(vmem_limit_bytes=8 * 2**20),
        name="notes",
    )(posted, twin)


def pack_first(grads, rows, count):
    vmem = pl.BlockSpec(memory_space=pltpu.VMEM)
    return pl.pallas_call(
        first_kernel,
        out_shape=[jax.ShapeDtypeStruct((rows, grads.shape[-1]), grads.dtype)] * count,
        in_specs=[pl.BlockSpec(memory_space=pltpu.HBM)],
        out_specs=[vmem] * count,
        scratch_shapes=[pltpu.SemaphoreType.DMA((count,))],
        compiler_params=pltpu.CompilerParams(vmem_limit_bytes=8 * 2**20),
        name="pack_first",
    )(pltpu.with_memory_space_constraint(grads, pltpu.HBM))


def pack_second(grads, offsets, given):
    rows, width = given[0].shape
    count = 2 * square - len(given)
    vmem = pl.BlockSpec(memory_space=pltpu.VMEM)
    block = jax.ShapeDtypeStruct((rows, width), grads.dtype)
    posted = jax.ShapeDtypeStruct((2 * offsets.shape[0], rows), jnp.int32)
    return pl.pallas_call(
        functools.partial(second_kernel, len(given)),
        out_shape=[block] * count + [posted],
        in_specs=[pl.BlockSpec(memory_space=pltpu.HBM)] + [vmem] * (1 + len(given)),
        out_specs=[vmem] * (count + 1),
        scratch_shapes=[pltpu.SemaphoreType.DMA((count,))],
        compiler_params=pltpu.CompilerParams(vmem_limit_bytes=8 * 2**20),
        name="pack_second",
    )(pltpu.with_memory_space_constraint(grads, pltpu.HBM), offsets, *given)


def noise_of(codes, columns):
    mixed = codes + columns
    mixed = jnp.bitwise_xor(mixed, jnp.right_shift(mixed, 13))
    mixed = mixed * 1103515245
    mixed = jnp.bitwise_xor(mixed, jnp.right_shift(mixed, 16))
    return jnp.bitwise_and(jnp.right_shift(mixed, 12), 255).astype(jnp.float32) * (1.0 / 256.0)


def fill_codes(far, mine, aside, above, codes):
    rows = [mine[far : far + 1, :], above[far : far + 1, :]]
    rows += [aside[far : far + 1, :], above[far + 2 : far + 3, :]]
    if far:
        inner = is_inner(lax.axis_index("dp")) == 1
        here, y, z, diagonal = rows
        rows = [jnp.where(inner, diagonal, here), jnp.where(inner, z, y)]
        rows += [jnp.where(inner, here, z), jnp.where(inner, y, diagonal)]
    codes[...] = jnp.transpose(jnp.concatenate(rows * 2)) * 747796405 + 1013904223


def noise_kernel(mine, aside, above, out, codes):
    fill_codes(1, mine, aside, above, codes)
    height, width = 16, out.shape[2]
    columns = lax.broadcasted_iota(jnp.int32, (1, width), 1) * 747796405

    def step(index, carry):
        span = pl.ds(pl.multiple_of(index * height, height), height)
        for near in range(square):
            out[near, span, :] = noise_of(codes[span, near : near + 1], columns).astype(jnp.bfloat16)
        return carry

    lax.fori_loop(0, out.shape[1] // height, step, 0)


def far_noise(notes, rows, width):
    vmem = pl.BlockSpec(memory_space=pltpu.VMEM)
    return pl.pallas_call(
        noise_kernel,
        out_shape=jax.ShapeDtypeStruct((square, rows, width), jnp.bfloat16),
        in_specs=[vmem] * len(notes),
        out_specs=vmem,
        scratch_shapes=[pltpu.VMEM((rows, 2 * square), jnp.int32)],
        compiler_params=pltpu.CompilerParams(vmem_limit_bytes=8 * 2**20),
        name="noise",
    )(*notes)


def sum_kernel(far, rows, mine, upward, aside, above, *refs):
    me = lax.axis_index("dp")
    inner = is_inner(me) == 1
    if far:
        noise, stays, *raws, out = refs
        target = jnp.where(inner, me, me ^ 6)
    else:
        *raws, out, codes = refs
        target = me
        fill_codes(0, mine, aside, above, codes)
    counts = jnp.maximum(upward[square : square + 1, :], above[square : square + 1, :])
    lanes = lax.broadcasted_iota(jnp.int32, counts.shape, 1)
    reached = jnp.where(lanes == target, counts, 0).astype(jnp.float32)
    exponent = jnp.max(reached, axis=1, keepdims=True).astype(jnp.int32) + (low_power - level_bits)
    inverse_step = power_of_two(-exponent)
    height, width = 16, raws[0].shape[1]
    columns = lax.broadcasted_iota(jnp.int32, (1, width), 1) * 747796405

    def step(index, carry):
        span = pl.ds(pl.multiple_of(index * height, height), height)
        total = jnp.zeros((height, width), jnp.float32)
        for near in range(square):
            if far:
                drawn = noise[near, span, :].astype(jnp.float32)
            else:
                drawn = noise_of(codes[span, near : near + 1], columns)
            values = raws[near][span, :].astype(jnp.float32)
            if far and near == 0:
                values = jnp.where(inner, values, stays[span, :].astype(jnp.float32))
            scaled = values * inverse_step
            floor_part = jnp.floor(scaled)
            total = total + (floor_part + jnp.floor(scaled - floor_part + drawn))
        out[span, :] = total.astype(jnp.bfloat16)
        return carry

    lax.fori_loop(0, rows // height, step, 0)
    if out.shape[0] > rows:
        tail = (out.shape[0] - rows, width)
        out[rows:, :] = jnp.broadcast_to(power_of_two(exponent), tail).astype(jnp.bfloat16)


def sum_counts(far, notes, raws, extra):
    rows, width = raws[-1].shape
    vmem = pl.BlockSpec(memory_space=pltpu.VMEM)
    return pl.pallas_call(
        functools.partial(sum_kernel, far, rows),
        out_shape=jax.ShapeDtypeStruct((rows + extra, width), jnp.bfloat16),
        in_specs=[vmem] * (len(notes) + len(raws)),
        out_specs=vmem,
        scratch_shapes=[] if far else [pltpu.VMEM((rows, 2 * square), jnp.int32)],
        compiler_params=pltpu.CompilerParams(vmem_limit_bytes=8 * 2**20),
        name="sum_far" if far else "sum_near",
    )(*notes, *raws)


def update_kernel(dp_count, slots, own, beside, across, arrived, weight, *refs):
    mean, updated, step, means, news, size_out, sems, size_sem = refs
    place = lax.axis_index("expert")
    positions = lax.broadcasted_iota(jnp.int32, slots.shape, 1)
    turns = jnp.where(slots[...] == place, positions ^ place, 0).astype(jnp.float32)
    turn = jnp.max(turns, axis=1, keepdims=True)
    rows = arrived.shape[0]

    def nearby(span):
        held, swapped, crossed = (ref[span, :].astype(jnp.float32) for ref in (own, beside, across))
        return jnp.where(turn == 0, held, jnp.where(turn == 1, swapped, crossed))

    size = nearby(slice(rows, own.shape[0]))[0:1, :]
    size_out[...] = size[:, 0:1]
    size_copy = pltpu.make_async_copy(size_out, step, size_sem)
    size_copy.start()
    scale = size * (1.0 / dp_count)
    parts = sems.shape[1]
    height = rows // parts
    copies = [size_copy]
    for part in range(parts):
        span = slice(part * height, (part + 1) * height)
        averaged = (nearby(span) + arrived[span, :].astype(jnp.float32)) * scale
        means[span, :] = averaged
        news[span, :] = weight[0, span, :] - learn_rate * averaged
        for number, (source, target) in enumerate(((means, mean), (news, updated))):
            copy = pltpu.make_async_copy(
                source.at[pl.ds(part * height, height), :],
                target.at[0, pl.ds(part * height, height), :],
                sems.at[number, part],
            )
            copy.start()
            copies.append(copy)
    for copy in copies:
        copy.wait()


def update(slots, own, beside, across, arrived, weight, dp_count):
    rows, width = arrived.shape
    parts = 4
    vmem = pl.BlockSpec(memory_space=pltpu.VMEM)
    hbm = pl.BlockSpec(memory_space=pltpu.HBM)
    block = jax.ShapeDtypeStruct((1, rows, width), jnp.float32)
    return pl.pallas_call(
        functools.partial(update_kernel, dp_count),
        out_shape=(block, block, jax.ShapeDtypeStruct((1, 1), jnp.float32)),
        in_specs=[vmem] * 6,
        out_specs=(hbm, hbm, hbm),
        scratch_shapes=[
            pltpu.VMEM((rows, width), jnp.float32),
            pltpu.VMEM((rows, width), jnp.float32),
            pltpu.VMEM((1, 1), jnp.float32),
            pltpu.SemaphoreType.DMA((2, parts)),
            pltpu.SemaphoreType.DMA,
        ],
        compiler_params=pltpu.CompilerParams(vmem_limit_bytes=8 * 2**20),
        name="update",
    )(slots[None], own, beside, across, arrived, weight)


def staged_body(expert_grads, round_offsets, slot_expert, master_weight):
    dp_count = lax.axis_size("dp")
    expert_count = lax.axis_size("expert")
    row_count, hidden = expert_grads.shape[2:]
    block_rows = row_count // dp_count
    place = lax.axis_index("expert")
    offsets = round_offsets[0, 0].reshape(dp_count, block_rows)

    after = jnp.arange(expert_count)[None, :] > jnp.arange(expert_count)[:, None]
    weights = jnp.array([6, 2, 1, 0], jnp.int32)[:, None]
    lower = (slot_expert[:, None] > slot_expert[None, :]) & after
    branch = jnp.sum(jnp.where(lower, weights, 0))
    first_blocks = pack_first(expert_grads, block_rows, 3)
    packed = pack_second(expert_grads, offsets, first_blocks)
    here, diagonal, four, five, last, posted = packed
    raw, fa = [here, first_blocks[0], first_blocks[1], diagonal], first_blocks[2]
    for near in range(1, square):
        raw[near] = lax.ppermute(raw[near], "dp", flips(dp_count, near))

    def mixed(inner_turn, outer_turn):
        turns = [inner_turn if is_inner(index) else outer_turn for index in range(dp_count)]
        return [(index, index ^ turn) for index, turn in enumerate(turns) if turn]

    fa = lax.ppermute(fa, "dp", mixed(6, 1))
    four = lax.ppermute(four, "dp", mixed(2, 4))
    five = lax.ppermute(five, "dp", mixed(3, 5))
    crossed = lax.ppermute(last, "dp", mixed(7, 0))

    twin = lax.ppermute(posted, "dp", flips(dp_count, square))
    mine, sideways = make_notes(posted, twin)
    aside = lax.ppermute(sideways, "dp", flips(dp_count, 2))
    levels = jnp.maximum(mine[square:], aside[square:])
    upward = jnp.concatenate([mine[2:square], aside[2:square], levels])
    above = lax.ppermute(upward, "dp", flips(dp_count, 1))
    noise = far_noise((mine, aside, above), block_rows, hidden)

    wanted = slot_expert == (place ^ 2)
    crossing = jnp.sum(jnp.where(wanted, jnp.arange(expert_count), 0)) == place
    own = sum_counts(0, (mine, upward, aside, above), raw, 8)
    beside = lax.ppermute(own, "expert", flips(expert_count, 1))
    across_wants = jnp.where(crossing, own, beside)
    across = lax.ppermute(across_wants, "expert", flips(expert_count, 2))
    raws = (noise, last, crossed, fa, four, five)
    message = sum_counts(1, (mine, upward, aside, above), raws, 0)

    def route(order):
        pairs = [
            (block * expert_count + slot, (block if is_inner(block) else block ^ 6) * expert_count + order[slot])
            for block in range(dp_count)
            for slot in range(expert_count)
        ]
        return lambda parts: lax.ppermute(parts, ("dp", "expert"), pairs)

    orders = itertools.permutations(range(expert_count))
    arrived = lax.switch(branch, [route(order) for order in orders], message)
    return update(slot_expert, own, beside, across, arrived, master_weight, dp_count)


def solution(mesh):
    staged = mesh.shape["dp"] == 2 * square and mesh.shape["expert"] == 4
    return jax.shard_map(
        staged_body if staged else general_body,
        mesh=mesh,
        in_specs=(
            P("dp", "expert", None, None),
            P("dp", "expert", None),
            P(),
            P("expert", "dp", None),
        ),
        out_specs=(P("expert", "dp", None), P("expert", "dp", None), P("expert", "dp")),
        check_vma=False,
    )
```

```python
import functools
import itertools

import jax
import jax.numpy as jnp
from jax import lax
from jax.experimental import pallas as pl
from jax.experimental.pallas import tpu as pltpu
from jax.sharding import PartitionSpec as P

level_bits = 6
low_power = -30
high_power = 30
learn_rate = 0.05
field_base = 32768
count_shift = 64
square = 4


def power_steps(maxima):
    powers = jnp.array([2.0**exponent for exponent in range(low_power, high_power)], jnp.float32)
    reached = maxima[..., None] >= powers
    doubled = jnp.prod(jnp.where(reached, jnp.float32(2.0), jnp.float32(1.0)), axis=-1)
    return 2.0 ** (low_power - level_bits) * doubled


def dither(element_code):
    mixed = element_code * 747796405 + 1013904223
    mixed = jnp.bitwise_xor(mixed, jnp.right_shift(mixed, 13))
    mixed = mixed * 1103515245
    mixed = jnp.bitwise_xor(mixed, jnp.right_shift(mixed, 16))
    return jnp.bitwise_and(jnp.right_shift(mixed, 12), 255).astype(jnp.float32) / 256.0


def quantize(values, inverse_step, offsets):
    columns = lax.broadcasted_iota(jnp.int32, (1, values.shape[-1]), 1)
    element_code = offsets[..., None] + columns
    scaled = values.astype(jnp.float32) * inverse_step
    floor_part = jnp.floor(scaled)
    return floor_part + jnp.floor(scaled - floor_part + dither(element_code))


def apply_update(mean_grad, master_weight):
    return mean_grad, master_weight - learn_rate * mean_grad


def general_body(expert_grads, round_offsets, slot_expert, master_weight):
    dp_count = lax.axis_size("dp")
    local_grads = expert_grads[0]
    slot_count, row_count, hidden = local_grads.shape
    block_rows = row_count // dp_count
    shaped = local_grads.reshape(slot_count, dp_count, block_rows, hidden)
    maxima = lax.pmax(jnp.max(jnp.abs(shaped), axis=(2, 3)).astype(jnp.float32), "dp")
    all_steps = power_steps(maxima)
    counts = quantize(
        shaped,
        (1.0 / all_steps)[:, :, None, None],
        round_offsets[0].reshape(slot_count, dp_count, block_rows),
    ).astype(jnp.int32).reshape(slot_count, row_count, hidden)
    half = hidden // 2
    words = (counts[:, :, :half] + count_shift) * field_base + (counts[:, :, half:] + count_shift)
    summed = lax.psum_scatter(words, "dp", scatter_dimension=1, tiled=True)
    upper = jnp.right_shift(summed, 15) - count_shift * dp_count
    lower = jnp.bitwise_and(summed, field_base - 1) - count_shift * dp_count
    totals = jnp.concatenate([upper, lower], axis=2)
    step_sizes = lax.dynamic_slice_in_dim(all_steps, lax.axis_index("dp"), 1, 1)
    mean_slot = totals.astype(jnp.float32) * (step_sizes / dp_count)[..., None]
    gathered = lax.all_gather(mean_slot, "expert", axis=0, tiled=True)
    gathered_steps = lax.all_gather(step_sizes, "expert", axis=0, tiled=True)
    wanted = lax.axis_index("expert") * slot_count + lax.broadcasted_iota(
        jnp.int32, (slot_count, 1), 0
    )
    positions = lax.broadcasted_iota(jnp.int32, (1, slot_expert.shape[0]), 1)
    holder = jnp.sum(jnp.where(slot_expert[None, :] == wanted, positions, 0), axis=1)
    mean_grad, new_weight = apply_update(gathered[holder], master_weight)
    return mean_grad, new_weight, gathered_steps[holder]


def flips(count, mask):
    return [(index, index ^ mask) for index in range(count)]


def power_of_two(exponent):
    result = jnp.ones(exponent.shape, jnp.float32)
    size = jnp.abs(exponent)
    for bit in range(6):
        factor = jnp.where(exponent < 0, jnp.float32(2.0 ** -(2**bit)), jnp.float32(2.0 ** (2**bit)))
        result = result * jnp.where((size >> bit) & 1 == 1, factor, jnp.float32(1.0))
    return result


def block_at(grads, target, rows):
    return grads.at[0, 0, pl.ds(pl.multiple_of(target * rows, rows), rows), :]


def largest(ref):
    height = 16
    best = jnp.abs(ref[0:height, :])
    for row in range(height, ref.shape[0], height):
        best = jnp.maximum(best, jnp.abs(ref[row : row + height, :]))
    best = jnp.max(best.astype(jnp.float32), axis=0, keepdims=True)
    return jnp.max(best, axis=1, keepdims=True)


def is_inner(index):
    return ((index >> 1) ^ (index >> 2)) & 1


def first_kernel(grads, *refs):
    outs, sems = refs[:-1], refs[-1]
    me = lax.axis_index("dp")
    copies = []
    targets = [me ^ 1, me ^ 2, me ^ (7 - is_inner(me))]
    for number, out in enumerate(outs):
        source = block_at(grads, targets[number], out.shape[0])
        copies.append(pltpu.make_async_copy(source, out, sems.at[number]))
        copies[-1].start()
    for copy in copies:
        copy.wait()


def second_kernel(given_count, grads, offsets, *refs):
    given, outs, (posted, sems) = refs[:given_count], refs[given_count:-2], refs[-2:]
    me = lax.axis_index("dp")
    inner = is_inner(me)
    targets = [me ^ turn for turn in (0, 3, 4, 5)] + [me ^ (6 + inner)]
    sources = [me ^ 1, me ^ 2, me ^ (7 - inner)]
    copies = []
    for number, target in enumerate(targets):
        source = block_at(grads, target, outs[number].shape[0])
        copies.append(pltpu.make_async_copy(source, outs[number], sems.at[number]))
        copies[-1].start()
    count = offsets.shape[0]
    posted[0:count, :] = offsets[...]
    lanes = lax.broadcasted_iota(jnp.int32, offsets.shape, 1)
    peaks = jnp.zeros(offsets.shape, jnp.float32)
    for number in range(given_count):
        peaks = jnp.where(lanes == sources[number], largest(given[number]), peaks)
    for number, target in enumerate(targets):
        copies[number].wait()
        peaks = jnp.where(lanes == target, largest(outs[number]), peaks)
    counts = [jnp.zeros(offsets.shape, jnp.int32) for _ in range(4)]
    for power in range(low_power, high_power):
        counts[power % 4] += (peaks >= jnp.float32(2.0**power)).astype(jnp.int32)
    posted[count:, :] = (counts[0] + counts[1]) + (counts[2] + counts[3])


def note_kernel(posted, twin, mine, aside):
    me = lax.axis_index("dp")
    count = posted.shape[0] // 2

    def fill(out, row, target):
        out[row : row + 1, :] = posted[pl.ds(target, 1), :]
        far = posted[pl.ds(target ^ 6, 1), :]
        out[row + 1 : row + 2, :] = jnp.where(is_inner(target) == 1, twin[pl.ds(target, 1), :], far)

    levels = jnp.maximum(posted[count : count + 4, :], twin[count : count + 4, :])
    for out, turn in ((mine, 0), (aside, 2)):
        fill(out, 0, me ^ turn)
        fill(out, 2, me ^ turn ^ 1)
        out[4:8, :] = levels


def make_notes(posted, twin):
    vmem = pl.BlockSpec(memory_space=pltpu.VMEM)
    note = jax.ShapeDtypeStruct((8, posted.shape[1]), jnp.int32)
    return pl.pallas_call(
        note_kernel,
        out_shape=[note] * 2,
        in_specs=[vmem] * 2,
        out_specs=[vmem] * 2,
        compiler_params=pltpu.CompilerParams(vmem_limit_bytes=8 * 2**20),
        name="notes",
    )(posted, twin)


def pack_first(grads, rows, count):
    vmem = pl.BlockSpec(memory_space=pltpu.VMEM)
    return pl.pallas_call(
        first_kernel,
        out_shape=[jax.ShapeDtypeStruct((rows, grads.shape[-1]), grads.dtype)] * count,
        in_specs=[pl.BlockSpec(memory_space=pltpu.HBM)],
        out_specs=[vmem] * count,
        scratch_shapes=[pltpu.SemaphoreType.DMA((count,))],
        compiler_params=pltpu.CompilerParams(vmem_limit_bytes=8 * 2**20),
        name="pack_first",
    )(pltpu.with_memory_space_constraint(grads, pltpu.HBM))


def pack_second(grads, offsets, given):
    rows, width = given[0].shape
    count = 2 * square - len(given)
    vmem = pl.BlockSpec(memory_space=pltpu.VMEM)
    block = jax.ShapeDtypeStruct((rows, width), grads.dtype)
    posted = jax.ShapeDtypeStruct((2 * offsets.shape[0], rows), jnp.int32)
    return pl.pallas_call(
        functools.partial(second_kernel, len(given)),
        out_shape=[block] * count + [posted],
        in_specs=[pl.BlockSpec(memory_space=pltpu.HBM)] + [vmem] * (1 + len(given)),
        out_specs=[vmem] * (count + 1),
        scratch_shapes=[pltpu.SemaphoreType.DMA((count,))],
        compiler_params=pltpu.CompilerParams(vmem_limit_bytes=8 * 2**20),
        name="pack_second",
    )(pltpu.with_memory_space_constraint(grads, pltpu.HBM), offsets, *given)


def noise_of(codes, columns):
    mixed = codes + columns
    mixed = jnp.bitwise_xor(mixed, jnp.right_shift(mixed, 13))
    mixed = mixed * 1103515245
    mixed = jnp.bitwise_xor(mixed, jnp.right_shift(mixed, 16))
    return jnp.bitwise_and(jnp.right_shift(mixed, 12), 255).astype(jnp.float32) * (1.0 / 256.0)


def fill_codes(far, mine, aside, above, codes):
    rows = [mine[far : far + 1, :], above[far : far + 1, :]]
    rows += [aside[far : far + 1, :], above[far + 2 : far + 3, :]]
    if far:
        inner = is_inner(lax.axis_index("dp")) == 1
        here, y, z, diagonal = rows
        rows = [jnp.where(inner, diagonal, here), jnp.where(inner, z, y)]
        rows += [jnp.where(inner, here, z), jnp.where(inner, y, diagonal)]
    codes[...] = jnp.transpose(jnp.concatenate(rows * 2)) * 747796405 + 1013904223


def noise_kernel(mine, aside, above, out, codes):
    fill_codes(1, mine, aside, above, codes)
    height, width = 32, out.shape[2]
    columns = lax.broadcasted_iota(jnp.int32, (1, width), 1) * 747796405

    def step(index, carry):
        span = pl.ds(pl.multiple_of(index * height, height), height)
        for near in range(square):
            out[near, span, :] = noise_of(codes[span, near : near + 1], columns).astype(jnp.bfloat16)
        return carry

    lax.fori_loop(0, out.shape[1] // height, step, 0)


def far_noise(notes, rows, width):
    vmem = pl.BlockSpec(memory_space=pltpu.VMEM)
    return pl.pallas_call(
        noise_kernel,
        out_shape=jax.ShapeDtypeStruct((square, rows, width), jnp.bfloat16),
        in_specs=[vmem] * len(notes),
        out_specs=vmem,
        scratch_shapes=[pltpu.VMEM((rows, 2 * square), jnp.int32)],
        compiler_params=pltpu.CompilerParams(vmem_limit_bytes=8 * 2**20),
        name="noise",
    )(*notes)


def sum_kernel(far, rows, mine, upward, aside, above, *refs):
    me = lax.axis_index("dp")
    inner = is_inner(me) == 1
    if far:
        noise, stays, *raws, out = refs
        target = jnp.where(inner, me, me ^ 6)
    else:
        *raws, out, codes = refs
        target = me
        fill_codes(0, mine, aside, above, codes)
    counts = jnp.maximum(upward[square : square + 1, :], above[square : square + 1, :])
    lanes = lax.broadcasted_iota(jnp.int32, counts.shape, 1)
    reached = jnp.where(lanes == target, counts, 0).astype(jnp.float32)
    exponent = jnp.max(reached, axis=1, keepdims=True).astype(jnp.int32) + (low_power - level_bits)
    inverse_step = power_of_two(-exponent)
    height, width = 32, raws[0].shape[1]
    columns = lax.broadcasted_iota(jnp.int32, (1, width), 1) * 747796405

    def step(index, carry):
        span = pl.ds(pl.multiple_of(index * height, height), height)
        total = jnp.zeros((height, width), jnp.float32)
        for near in range(square):
            if far:
                drawn = noise[near, span, :].astype(jnp.float32)
            else:
                drawn = noise_of(codes[span, near : near + 1], columns)
            values = raws[near][span, :].astype(jnp.float32)
            if far and near == 0:
                values = jnp.where(inner, values, stays[span, :].astype(jnp.float32))
            scaled = values * inverse_step
            floor_part = jnp.floor(scaled)
            total = total + (floor_part + jnp.floor(scaled - floor_part + drawn))
        out[span, :] = total.astype(jnp.bfloat16)
        return carry

    lax.fori_loop(0, rows // height, step, 0)
    if out.shape[0] > rows:
        tail = (out.shape[0] - rows, width)
        out[rows:, :] = jnp.broadcast_to(power_of_two(exponent), tail).astype(jnp.bfloat16)


def sum_counts(far, notes, raws, extra):
    rows, width = raws[-1].shape
    vmem = pl.BlockSpec(memory_space=pltpu.VMEM)
    return pl.pallas_call(
        functools.partial(sum_kernel, far, rows),
        out_shape=jax.ShapeDtypeStruct((rows + extra, width), jnp.bfloat16),
        in_specs=[vmem] * (len(notes) + len(raws)),
        out_specs=vmem,
        scratch_shapes=[] if far else [pltpu.VMEM((rows, 2 * square), jnp.int32)],
        compiler_params=pltpu.CompilerParams(vmem_limit_bytes=8 * 2**20),
        name="sum_far" if far else "sum_near",
    )(*notes, *raws)


def choose_kernel(slots, own, beside, out):
    place = lax.axis_index("expert")
    positions = lax.broadcasted_iota(jnp.int32, slots.shape, 1)
    wanted = jnp.where(positions == place, slots[...], -1) == (place ^ 2)
    holds = jnp.max(wanted.astype(jnp.float32), axis=1, keepdims=True)
    height = 8

    def step(index, carry):
        span = pl.ds(pl.multiple_of(index * height, height), height)
        held, swapped = own[span, :].astype(jnp.float32), beside[span, :].astype(jnp.float32)
        out[span, :] = jnp.where(holds > 0, held, swapped).astype(out.dtype)
        return carry

    lax.fori_loop(0, out.shape[0] // height, step, 0)


def choose(slots, own, beside):
    vmem = pl.BlockSpec(memory_space=pltpu.VMEM)
    return pl.pallas_call(
        choose_kernel,
        out_shape=jax.ShapeDtypeStruct(own.shape, own.dtype),
        in_specs=[vmem] * 3,
        out_specs=vmem,
        compiler_params=pltpu.CompilerParams(vmem_limit_bytes=8 * 2**20),
        name="choose",
    )(slots[None], own, beside)


def update_kernel(dp_count, slots, own, beside, across, arrived, weight, *refs):
    mean, updated, step, landed, means, news, size_out, sems, size_sem = refs
    rows = arrived.shape[0]
    parts = sems.shape[1]
    height = rows // parts

    def strip(part):
        return pl.ds(pl.multiple_of(part * height, height), height)

    def fetch(part):
        return pltpu.make_async_copy(arrived.at[strip(part), :], landed.at[strip(part), :], sems.at[2, part])

    for part in range(parts):
        fetch(part).start()
    place = lax.axis_index("expert")
    positions = lax.broadcasted_iota(jnp.int32, slots.shape, 1)
    turns = jnp.where(slots[...] == place, positions ^ place, 0).astype(jnp.float32)
    turn = jnp.max(turns, axis=1, keepdims=True)

    def nearby(span):
        held, swapped, crossed = (ref[span, :].astype(jnp.float32) for ref in (own, beside, across))
        return jnp.where(turn == 0, held, jnp.where(turn == 1, swapped, crossed))

    size = nearby(slice(rows, own.shape[0]))[0:1, :]
    size_out[...] = size[:, 0:1]
    size_copy = pltpu.make_async_copy(size_out, step, size_sem)
    size_copy.start()
    scale = size * (1.0 / dp_count)

    def copies(part):
        span = strip(part)
        return [
            pltpu.make_async_copy(source.at[span, :], target.at[0, span, :], sems.at[number, part])
            for number, (source, target) in enumerate(((means, mean), (news, updated)))
        ]

    def step_part(part, carry):
        span = strip(part)
        fetch(part).wait()
        averaged = (nearby(span) + landed[span, :].astype(jnp.float32)) * scale
        means[span, :] = averaged
        news[span, :] = weight[0, span, :] - learn_rate * averaged
        for copy in copies(part):
            copy.start()
        return carry

    def wait_part(part, carry):
        for copy in copies(part):
            copy.wait()
        return carry

    lax.fori_loop(0, parts, step_part, 0)
    lax.fori_loop(0, parts, wait_part, 0)
    size_copy.wait()


def update(slots, own, beside, across, arrived, weight, dp_count):
    rows, width = arrived.shape
    parts = 4
    vmem = pl.BlockSpec(memory_space=pltpu.VMEM)
    hbm = pl.BlockSpec(memory_space=pltpu.HBM)
    block = jax.ShapeDtypeStruct((1, rows, width), jnp.float32)
    return pl.pallas_call(
        functools.partial(update_kernel, dp_count),
        out_shape=(block, block, jax.ShapeDtypeStruct((1, 1), jnp.float32)),
        in_specs=[vmem] * 4 + [hbm, vmem],
        out_specs=(hbm, hbm, hbm),
        scratch_shapes=[
            pltpu.VMEM((rows, width), arrived.dtype),
            pltpu.VMEM((rows, width), jnp.float32),
            pltpu.VMEM((rows, width), jnp.float32),
            pltpu.VMEM((1, 1), jnp.float32),
            pltpu.SemaphoreType.DMA((3, parts)),
            pltpu.SemaphoreType.DMA,
        ],
        compiler_params=pltpu.CompilerParams(vmem_limit_bytes=8 * 2**20),
        name="update",
    )(slots[None], own, beside, across, arrived, weight)


def staged_body(expert_grads, round_offsets, slot_expert, master_weight):
    dp_count = lax.axis_size("dp")
    expert_count = lax.axis_size("expert")
    row_count, hidden = expert_grads.shape[2:]
    block_rows = row_count // dp_count
    offsets = round_offsets[0, 0].reshape(dp_count, block_rows)

    after = jnp.arange(expert_count)[None, :] > jnp.arange(expert_count)[:, None]
    weights = jnp.array([6, 2, 1, 0], jnp.int32)[:, None]
    lower = (slot_expert[:, None] > slot_expert[None, :]) & after
    branch = jnp.sum(jnp.where(lower, weights, 0))
    first_blocks = pack_first(expert_grads, block_rows, 3)
    packed = pack_second(expert_grads, offsets, first_blocks)
    here, diagonal, four, five, last, posted = packed
    raw, fa = [here, first_blocks[0], first_blocks[1], diagonal], first_blocks[2]
    for near in range(1, square):
        raw[near] = lax.ppermute(raw[near], "dp", flips(dp_count, near))

    def mixed(inner_turn, outer_turn):
        turns = [inner_turn if is_inner(index) else outer_turn for index in range(dp_count)]
        return [(index, index ^ turn) for index, turn in enumerate(turns) if turn]

    fa = lax.ppermute(fa, "dp", mixed(6, 1))
    four = lax.ppermute(four, "dp", mixed(2, 4))
    five = lax.ppermute(five, "dp", mixed(3, 5))
    crossed = lax.ppermute(last, "dp", mixed(7, 0))

    twin = lax.ppermute(posted, "dp", flips(dp_count, square))
    mine, sideways = make_notes(posted, twin)
    aside = lax.ppermute(sideways, "dp", flips(dp_count, 2))
    levels = jnp.maximum(mine[square:], aside[square:])
    upward = jnp.concatenate([mine[2:square], aside[2:square], levels])
    above = lax.ppermute(upward, "dp", flips(dp_count, 1))
    noise = far_noise((mine, aside, above), block_rows, hidden)

    own = sum_counts(0, (mine, upward, aside, above), raw, 8)
    beside = lax.ppermute(own, "expert", flips(expert_count, 1))
    across = lax.ppermute(choose(slot_expert, own, beside), "expert", flips(expert_count, 2))
    raws = (noise, last, crossed, fa, four, five)
    message = sum_counts(1, (mine, upward, aside, above), raws, 0)

    def route(order):
        pairs = [
            (block * expert_count + slot, (block if is_inner(block) else block ^ 6) * expert_count + order[slot])
            for block in range(dp_count)
            for slot in range(expert_count)
        ]
        return lambda parts: lax.ppermute(parts, ("dp", "expert"), pairs)

    orders = itertools.permutations(range(expert_count))
    arrived = lax.switch(branch, [route(order) for order in orders], message)
    return update(slot_expert, own, beside, across, arrived, master_weight, dp_count)


def solution(mesh):
    staged = mesh.shape["dp"] == 2 * square and mesh.shape["expert"] == 4
    return jax.shard_map(
        staged_body if staged else general_body,
        mesh=mesh,
        in_specs=(
            P("dp", "expert", None, None),
            P("dp", "expert", None),
            P(),
            P("expert", "dp", None),
        ),
        out_specs=(P("expert", "dp", None), P("expert", "dp", None), P("expert", "dp")),
        check_vma=False,
    )
```

```python
import functools
import itertools

import jax
import jax.numpy as jnp
from jax import lax
from jax.experimental import pallas as pl
from jax.experimental.pallas import tpu as pltpu
from jax.sharding import PartitionSpec as P

level_bits = 6
low_power = -30
high_power = 30
learn_rate = 0.05
field_base = 32768
count_shift = 64
square = 4


def power_steps(maxima):
    powers = jnp.array([2.0**exponent for exponent in range(low_power, high_power)], jnp.float32)
    reached = maxima[..., None] >= powers
    doubled = jnp.prod(jnp.where(reached, jnp.float32(2.0), jnp.float32(1.0)), axis=-1)
    return 2.0 ** (low_power - level_bits) * doubled


def dither(element_code):
    mixed = element_code * 747796405 + 1013904223
    mixed = jnp.bitwise_xor(mixed, jnp.right_shift(mixed, 13))
    mixed = mixed * 1103515245
    mixed = jnp.bitwise_xor(mixed, jnp.right_shift(mixed, 16))
    return jnp.bitwise_and(jnp.right_shift(mixed, 12), 255).astype(jnp.float32) / 256.0


def quantize(values, inverse_step, offsets):
    columns = lax.broadcasted_iota(jnp.int32, (1, values.shape[-1]), 1)
    element_code = offsets[..., None] + columns
    scaled = values.astype(jnp.float32) * inverse_step
    floor_part = jnp.floor(scaled)
    return floor_part + jnp.floor(scaled - floor_part + dither(element_code))


def apply_update(mean_grad, master_weight):
    return mean_grad, master_weight - learn_rate * mean_grad


def general_body(expert_grads, round_offsets, slot_expert, master_weight):
    dp_count = lax.axis_size("dp")
    local_grads = expert_grads[0]
    slot_count, row_count, hidden = local_grads.shape
    block_rows = row_count // dp_count
    shaped = local_grads.reshape(slot_count, dp_count, block_rows, hidden)
    maxima = lax.pmax(jnp.max(jnp.abs(shaped), axis=(2, 3)).astype(jnp.float32), "dp")
    all_steps = power_steps(maxima)
    counts = quantize(
        shaped,
        (1.0 / all_steps)[:, :, None, None],
        round_offsets[0].reshape(slot_count, dp_count, block_rows),
    ).astype(jnp.int32).reshape(slot_count, row_count, hidden)
    half = hidden // 2
    words = (counts[:, :, :half] + count_shift) * field_base + (counts[:, :, half:] + count_shift)
    summed = lax.psum_scatter(words, "dp", scatter_dimension=1, tiled=True)
    upper = jnp.right_shift(summed, 15) - count_shift * dp_count
    lower = jnp.bitwise_and(summed, field_base - 1) - count_shift * dp_count
    totals = jnp.concatenate([upper, lower], axis=2)
    step_sizes = lax.dynamic_slice_in_dim(all_steps, lax.axis_index("dp"), 1, 1)
    mean_slot = totals.astype(jnp.float32) * (step_sizes / dp_count)[..., None]
    gathered = lax.all_gather(mean_slot, "expert", axis=0, tiled=True)
    gathered_steps = lax.all_gather(step_sizes, "expert", axis=0, tiled=True)
    wanted = lax.axis_index("expert") * slot_count + lax.broadcasted_iota(
        jnp.int32, (slot_count, 1), 0
    )
    positions = lax.broadcasted_iota(jnp.int32, (1, slot_expert.shape[0]), 1)
    holder = jnp.sum(jnp.where(slot_expert[None, :] == wanted, positions, 0), axis=1)
    mean_grad, new_weight = apply_update(gathered[holder], master_weight)
    return mean_grad, new_weight, gathered_steps[holder]


def flips(count, mask):
    return [(index, index ^ mask) for index in range(count)]


def power_of_two(exponent):
    result = jnp.ones(exponent.shape, jnp.float32)
    size = jnp.abs(exponent)
    for bit in range(6):
        factor = jnp.where(exponent < 0, jnp.float32(2.0 ** -(2**bit)), jnp.float32(2.0 ** (2**bit)))
        result = result * jnp.where((size >> bit) & 1 == 1, factor, jnp.float32(1.0))
    return result


def block_at(grads, target, rows):
    return grads.at[0, 0, pl.ds(pl.multiple_of(target * rows, rows), rows), :]


def largest(ref):
    height = 16
    best = jnp.abs(ref[0:height, :])
    for row in range(height, ref.shape[0], height):
        best = jnp.maximum(best, jnp.abs(ref[row : row + height, :]))
    best = jnp.max(best.astype(jnp.float32), axis=0, keepdims=True)
    return jnp.max(best, axis=1, keepdims=True)


def is_inner(index):
    return ((index >> 1) ^ (index >> 2)) & 1


def first_kernel(grads, *refs):
    outs, sems = refs[:-1], refs[-1]
    me = lax.axis_index("dp")
    copies = []
    targets = [me ^ 1, me ^ 2, me ^ (7 - is_inner(me))]
    for number, out in enumerate(outs):
        source = block_at(grads, targets[number], out.shape[0])
        copies.append(pltpu.make_async_copy(source, out, sems.at[number]))
        copies[-1].start()
    for copy in copies:
        copy.wait()


def second_kernel(given_count, grads, offsets, *refs):
    given, outs, (posted, sems) = refs[:given_count], refs[given_count:-2], refs[-2:]
    me = lax.axis_index("dp")
    inner = is_inner(me)
    targets = [me ^ turn for turn in (0, 3, 4, 5)] + [me ^ (6 + inner)]
    sources = [me ^ 1, me ^ 2, me ^ (7 - inner)]
    copies = []
    for number, target in enumerate(targets):
        source = block_at(grads, target, outs[number].shape[0])
        copies.append(pltpu.make_async_copy(source, outs[number], sems.at[number]))
        copies[-1].start()
    count = offsets.shape[0]
    posted[0:count, :] = offsets[...]
    lanes = lax.broadcasted_iota(jnp.int32, offsets.shape, 1)
    peaks = jnp.zeros(offsets.shape, jnp.float32)
    for number in range(given_count):
        peaks = jnp.where(lanes == sources[number], largest(given[number]), peaks)
    for number, target in enumerate(targets):
        copies[number].wait()
        peaks = jnp.where(lanes == target, largest(outs[number]), peaks)
    counts = [jnp.zeros(offsets.shape, jnp.int32) for _ in range(4)]
    for power in range(low_power, high_power):
        counts[power % 4] += (peaks >= jnp.float32(2.0**power)).astype(jnp.int32)
    posted[count:, :] = (counts[0] + counts[1]) + (counts[2] + counts[3])


def note_kernel(posted, twin, mine, aside):
    me = lax.axis_index("dp")
    count = posted.shape[0] // 2

    def fill(out, row, target):
        out[row : row + 1, :] = posted[pl.ds(target, 1), :]
        far = posted[pl.ds(target ^ 6, 1), :]
        out[row + 1 : row + 2, :] = jnp.where(is_inner(target) == 1, twin[pl.ds(target, 1), :], far)

    levels = jnp.maximum(posted[count : count + 4, :], twin[count : count + 4, :])
    for out, turn in ((mine, 0), (aside, 2)):
        fill(out, 0, me ^ turn)
        fill(out, 2, me ^ turn ^ 1)
        out[4:8, :] = levels


def make_notes(posted, twin):
    vmem = pl.BlockSpec(memory_space=pltpu.VMEM)
    note = jax.ShapeDtypeStruct((8, posted.shape[1]), jnp.int32)
    return pl.pallas_call(
        note_kernel,
        out_shape=[note] * 2,
        in_specs=[vmem] * 2,
        out_specs=[vmem] * 2,
        compiler_params=pltpu.CompilerParams(vmem_limit_bytes=8 * 2**20),
        name="notes",
    )(posted, twin)


def pack_first(grads, rows, count):
    vmem = pl.BlockSpec(memory_space=pltpu.VMEM)
    return pl.pallas_call(
        first_kernel,
        out_shape=[jax.ShapeDtypeStruct((rows, grads.shape[-1]), grads.dtype)] * count,
        in_specs=[pl.BlockSpec(memory_space=pltpu.HBM)],
        out_specs=[vmem] * count,
        scratch_shapes=[pltpu.SemaphoreType.DMA((count,))],
        compiler_params=pltpu.CompilerParams(vmem_limit_bytes=8 * 2**20),
        name="pack_first",
    )(pltpu.with_memory_space_constraint(grads, pltpu.HBM))


def pack_second(grads, offsets, given):
    rows, width = given[0].shape
    count = 2 * square - len(given)
    vmem = pl.BlockSpec(memory_space=pltpu.VMEM)
    block = jax.ShapeDtypeStruct((rows, width), grads.dtype)
    posted = jax.ShapeDtypeStruct((2 * offsets.shape[0], rows), jnp.int32)
    return pl.pallas_call(
        functools.partial(second_kernel, len(given)),
        out_shape=[block] * count + [posted],
        in_specs=[pl.BlockSpec(memory_space=pltpu.HBM)] + [vmem] * (1 + len(given)),
        out_specs=[vmem] * (count + 1),
        scratch_shapes=[pltpu.SemaphoreType.DMA((count,))],
        compiler_params=pltpu.CompilerParams(vmem_limit_bytes=8 * 2**20),
        name="pack_second",
    )(pltpu.with_memory_space_constraint(grads, pltpu.HBM), offsets, *given)


def noise_of(codes, columns):
    mixed = codes + columns
    mixed = jnp.bitwise_xor(mixed, jnp.right_shift(mixed, 13))
    mixed = mixed * 1103515245
    mixed = jnp.bitwise_xor(mixed, jnp.right_shift(mixed, 16))
    return jnp.bitwise_and(jnp.right_shift(mixed, 12), 255).astype(jnp.float32) * (1.0 / 256.0)


def fill_codes(rows, codes):
    spare = [rows[0]] * (codes.shape[1] - len(rows))
    codes[...] = jnp.transpose(jnp.concatenate(rows + spare)) * 747796405 + 1013904223


def noise_kernel(picks, *refs):
    notes, out, codes = refs[:-2], refs[-2], refs[-1]
    fill_codes([notes[note][row : row + 1, :] for note, row in picks], codes)
    height, width = 32, out.shape[2]
    columns = lax.broadcasted_iota(jnp.int32, (1, width), 1) * 747796405

    def step(index, carry):
        span = pl.ds(pl.multiple_of(index * height, height), height)
        for slab in range(len(picks)):
            out[slab, span, :] = noise_of(codes[span, slab : slab + 1], columns).astype(jnp.bfloat16)
        return carry

    lax.fori_loop(0, out.shape[1] // height, step, 0)


def draw_noise(picks, notes, rows, width):
    vmem = pl.BlockSpec(memory_space=pltpu.VMEM)
    return pl.pallas_call(
        functools.partial(noise_kernel, picks),
        out_shape=jax.ShapeDtypeStruct((len(picks), rows, width), jnp.bfloat16),
        in_specs=[vmem] * len(notes),
        out_specs=vmem,
        scratch_shapes=[pltpu.VMEM((rows, 2 * square), jnp.int32)],
        compiler_params=pltpu.CompilerParams(vmem_limit_bytes=8 * 2**20),
        name="noise",
    )(*notes)


def sum_kernel(far, rows, upward, above, early, *refs):
    me = lax.axis_index("dp")
    inner = is_inner(me) == 1
    if far:
        late, stays, *raws, out = refs
        target = jnp.where(inner, me, me ^ 6)
    else:
        *raws, out, codes = refs
        target = me
        fill_codes([above[0:1, :], above[2:3, :]], codes)
    counts = jnp.maximum(upward[square : square + 1, :], above[square : square + 1, :])
    lanes = lax.broadcasted_iota(jnp.int32, counts.shape, 1)
    reached = jnp.where(lanes == target, counts, 0).astype(jnp.float32)
    exponent = jnp.max(reached, axis=1, keepdims=True).astype(jnp.int32) + (low_power - level_bits)
    inverse_step = power_of_two(-exponent)
    slabs = [early.at[2], early.at[3], late.at[0], late.at[1]] if far else []
    height, width = 32, raws[0].shape[1]
    columns = lax.broadcasted_iota(jnp.int32, (1, width), 1) * 747796405

    def step(index, carry):
        span = pl.ds(pl.multiple_of(index * height, height), height)
        total = jnp.zeros((height, width), jnp.float32)
        if far:
            here, z, y, diagonal = (slab[span, :].astype(jnp.float32) for slab in slabs)
            chosen = ((diagonal, here), (z, y), (here, z), (y, diagonal))
            noises = [jnp.where(inner, *pair) for pair in chosen]
        else:
            here, z = (early[slab, span, :].astype(jnp.float32) for slab in range(2))
            y, diagonal = (noise_of(codes[span, column : column + 1], columns) for column in range(2))
            noises = [here, y, z, diagonal]
        for near in range(square):
            drawn = noises[near]
            values = raws[near][span, :].astype(jnp.float32)
            if far and near == 0:
                values = jnp.where(inner, values, stays[span, :].astype(jnp.float32))
            scaled = values * inverse_step
            floor_part = jnp.floor(scaled)
            total = total + (floor_part + jnp.floor(scaled - floor_part + drawn))
        out[span, :] = total.astype(jnp.bfloat16)
        return carry

    lax.fori_loop(0, rows // height, step, 0)
    if out.shape[0] > rows:
        tail = (out.shape[0] - rows, width)
        out[rows:, :] = jnp.broadcast_to(power_of_two(exponent), tail).astype(jnp.bfloat16)


def sum_counts(far, notes, raws, extra):
    rows, width = raws[-1].shape
    vmem = pl.BlockSpec(memory_space=pltpu.VMEM)
    return pl.pallas_call(
        functools.partial(sum_kernel, far, rows),
        out_shape=jax.ShapeDtypeStruct((rows + extra, width), jnp.bfloat16),
        in_specs=[vmem] * (len(notes) + len(raws)),
        out_specs=vmem,
        scratch_shapes=[] if far else [pltpu.VMEM((rows, 2 * square), jnp.int32)],
        compiler_params=pltpu.CompilerParams(vmem_limit_bytes=8 * 2**20),
        name="sum_far" if far else "sum_near",
    )(*notes, *raws)


def choose_kernel(slots, own, beside, out):
    place = lax.axis_index("expert")
    positions = lax.broadcasted_iota(jnp.int32, slots.shape, 1)
    wanted = jnp.where(positions == place, slots[...], -1) == (place ^ 2)
    holds = jnp.max(wanted.astype(jnp.float32), axis=1, keepdims=True)
    height = 8

    def step(index, carry):
        span = pl.ds(pl.multiple_of(index * height, height), height)
        held, swapped = own[span, :].astype(jnp.float32), beside[span, :].astype(jnp.float32)
        out[span, :] = jnp.where(holds > 0, held, swapped).astype(out.dtype)
        return carry

    lax.fori_loop(0, out.shape[0] // height, step, 0)


def choose(slots, own, beside):
    vmem = pl.BlockSpec(memory_space=pltpu.VMEM)
    return pl.pallas_call(
        choose_kernel,
        out_shape=jax.ShapeDtypeStruct(own.shape, own.dtype),
        in_specs=[vmem] * 3,
        out_specs=vmem,
        compiler_params=pltpu.CompilerParams(vmem_limit_bytes=8 * 2**20),
        name="choose",
    )(slots[None], own, beside)


def update_kernel(dp_count, slots, own, beside, across, arrived, weight, *refs):
    mean, updated, step, landed, means, news, size_out, sems, size_sem = refs
    rows = arrived.shape[0]
    parts = sems.shape[1]
    height = rows // parts

    def strip(part):
        return pl.ds(pl.multiple_of(part * height, height), height)

    def fetch(part):
        return pltpu.make_async_copy(arrived.at[strip(part), :], landed.at[strip(part), :], sems.at[2, part])

    for part in range(parts):
        fetch(part).start()
    place = lax.axis_index("expert")
    positions = lax.broadcasted_iota(jnp.int32, slots.shape, 1)
    turns = jnp.where(slots[...] == place, positions ^ place, 0).astype(jnp.float32)
    turn = jnp.max(turns, axis=1, keepdims=True)

    def nearby(span):
        held, swapped, crossed = (ref[span, :].astype(jnp.float32) for ref in (own, beside, across))
        return jnp.where(turn == 0, held, jnp.where(turn == 1, swapped, crossed))

    size = nearby(slice(rows, own.shape[0]))[0:1, :]
    size_out[...] = size[:, 0:1]
    size_copy = pltpu.make_async_copy(size_out, step, size_sem)
    size_copy.start()
    scale = size * (1.0 / dp_count)

    def copies(part):
        span = strip(part)
        return [
            pltpu.make_async_copy(source.at[span, :], target.at[0, span, :], sems.at[number, part])
            for number, (source, target) in enumerate(((means, mean), (news, updated)))
        ]

    def step_part(part, carry):
        span = strip(part)
        fetch(part).wait()
        averaged = (nearby(span) + landed[span, :].astype(jnp.float32)) * scale
        means[span, :] = averaged
        news[span, :] = weight[0, span, :] - learn_rate * averaged
        for copy in copies(part):
            copy.start()
        return carry

    def wait_part(part, carry):
        for copy in copies(part):
            copy.wait()
        return carry

    lax.fori_loop(0, parts, step_part, 0)
    lax.fori_loop(0, parts, wait_part, 0)
    size_copy.wait()


def update(slots, own, beside, across, arrived, weight, dp_count):
    rows, width = arrived.shape
    parts = 4
    vmem = pl.BlockSpec(memory_space=pltpu.VMEM)
    hbm = pl.BlockSpec(memory_space=pltpu.HBM)
    block = jax.ShapeDtypeStruct((1, rows, width), jnp.float32)
    return pl.pallas_call(
        functools.partial(update_kernel, dp_count),
        out_shape=(block, block, jax.ShapeDtypeStruct((1, 1), jnp.float32)),
        in_specs=[vmem] * 4 + [hbm, vmem],
        out_specs=(hbm, hbm, hbm),
        scratch_shapes=[
            pltpu.VMEM((rows, width), arrived.dtype),
            pltpu.VMEM((rows, width), jnp.float32),
            pltpu.VMEM((rows, width), jnp.float32),
            pltpu.VMEM((1, 1), jnp.float32),
            pltpu.SemaphoreType.DMA((3, parts)),
            pltpu.SemaphoreType.DMA,
        ],
        compiler_params=pltpu.CompilerParams(vmem_limit_bytes=8 * 2**20),
        name="update",
    )(slots[None], own, beside, across, arrived, weight)


def staged_body(expert_grads, round_offsets, slot_expert, master_weight):
    dp_count = lax.axis_size("dp")
    expert_count = lax.axis_size("expert")
    row_count, hidden = expert_grads.shape[2:]
    block_rows = row_count // dp_count
    offsets = round_offsets[0, 0].reshape(dp_count, block_rows)

    after = jnp.arange(expert_count)[None, :] > jnp.arange(expert_count)[:, None]
    weights = jnp.array([6, 2, 1, 0], jnp.int32)[:, None]
    lower = (slot_expert[:, None] > slot_expert[None, :]) & after
    branch = jnp.sum(jnp.where(lower, weights, 0))
    first_blocks = pack_first(expert_grads, block_rows, 3)
    packed = pack_second(expert_grads, offsets, first_blocks)
    here, diagonal, four, five, last, posted = packed
    raw, fa = [here, first_blocks[0], first_blocks[1], diagonal], first_blocks[2]
    for near in range(1, square):
        raw[near] = lax.ppermute(raw[near], "dp", flips(dp_count, near))

    def mixed(inner_turn, outer_turn):
        turns = [inner_turn if is_inner(index) else outer_turn for index in range(dp_count)]
        return [(index, index ^ turn) for index, turn in enumerate(turns) if turn]

    fa = lax.ppermute(fa, "dp", mixed(6, 1))
    four = lax.ppermute(four, "dp", mixed(2, 4))
    five = lax.ppermute(five, "dp", mixed(3, 5))
    crossed = lax.ppermute(last, "dp", mixed(7, 0))

    twin = lax.ppermute(posted, "dp", flips(dp_count, square))
    mine, sideways = make_notes(posted, twin)
    aside = lax.ppermute(sideways, "dp", flips(dp_count, 2))
    levels = jnp.maximum(mine[square:], aside[square:])
    upward = jnp.concatenate([mine[2:square], aside[2:square], levels])
    above = lax.ppermute(upward, "dp", flips(dp_count, 1))
    picks = ((0, 0), (1, 0), (0, 1), (1, 1))
    early = draw_noise(picks, (mine, aside), block_rows, hidden)
    late = draw_noise(((0, 1), (0, 3)), (above,), block_rows, hidden)

    own = sum_counts(0, (upward, above, early), raw, 8)
    beside = lax.ppermute(own, "expert", flips(expert_count, 1))
    across = lax.ppermute(choose(slot_expert, own, beside), "expert", flips(expert_count, 2))
    raws = (late, last, crossed, fa, four, five)
    message = sum_counts(1, (upward, above, early), raws, 0)

    def route(order):
        pairs = [
            (block * expert_count + slot, (block if is_inner(block) else block ^ 6) * expert_count + order[slot])
            for block in range(dp_count)
            for slot in range(expert_count)
        ]
        return lambda parts: lax.ppermute(parts, ("dp", "expert"), pairs)

    orders = itertools.permutations(range(expert_count))
    arrived = lax.switch(branch, [route(order) for order in orders], message)
    return update(slot_expert, own, beside, across, arrived, master_weight, dp_count)


def solution(mesh):
    staged = mesh.shape["dp"] == 2 * square and mesh.shape["expert"] == 4
    return jax.shard_map(
        staged_body if staged else general_body,
        mesh=mesh,
        in_specs=(
            P("dp", "expert", None, None),
            P("dp", "expert", None),
            P(),
            P("expert", "dp", None),
        ),
        out_specs=(P("expert", "dp", None), P("expert", "dp", None), P("expert", "dp")),
        check_vma=False,
    )
```
